8 devices in a mesh: dp: 1 (over z), etp: 2 (over y), ep: 4 (over x, core).
Axes of the slice: x: 2, y: 2, z: 1, core: 2. Of those that a mesh axis runs over, the one named last changes fastest.
Arguments:
- x_in: bfloat16 [4096, 768], P(('dp', 'ep'))
- y_grad: bfloat16 [4096, 768], P(('dp', 'ep'))
- prim_exp: int32 [4096], P(('dp', 'ep'))
- alt_exp: int32 [4096], P(('dp', 'ep'))
- w_router: bfloat16 [768, 32], replicated
- exp_gate: bfloat16 [32, 768, 3072], P('ep', None, 'etp')
- exp_up: bfloat16 [32, 768, 3072], P('ep', None, 'etp')
- exp_down: bfloat16 [32, 3072, 768], P('ep', 'etp')
- sh_gate: bfloat16 [768, 3072], P(None, 'etp')
- sh_up: bfloat16 [768, 3072], P(None, 'etp')
- sh_down: bfloat16 [3072, 768], P('etp')
Outputs:
- output 1: bfloat16 [4096, 768], P(('dp', 'ep'))
- output 2: bfloat16 [4096, 768], P(('dp', 'ep'))
- output 3: float32 [32, 768, 3072], P(('dp', 'ep'), None, 'etp')
- output 4: float32 [32, 768, 3072], P(('dp', 'ep'), None, 'etp')
- output 5: float32 [32, 3072, 768], P(('dp', 'ep'), 'etp')
- output 6: float32 [768, 3072], P('dp', 'etp')
- output 7: float32 [768, 3072], P('dp', 'etp')
- output 8: float32 [3072, 768], P(('dp', 'etp'))
- output 9: float32 [768, 32], P('dp')
All inputs are finite; a program needn't handle non-finite values.
Results may differ from the reference program's by a relative error of at most 0.00507189.
Values are sent between devices in bfloat16 or wider.
A program may use at most 1 GiB of HBM per device.

```python
import jax
import jax.numpy as jnp
from jax import lax

D = 768
FF = 3072
EXPERTS = 32
TOKENS = 4096
CAP = 160
EPS = 1e-5


def draw_routes(route_key):
    key_hot, key_pick, key_coin, key_flat, key_alt = jax.random.split(route_key, 5)
    hot_ids = jax.random.permutation(key_hot, EXPERTS)[:3]
    hot_pick = jax.random.randint(key_pick, (TOKENS,), 0, 3)
    hot_coin = jax.random.randint(key_coin, (TOKENS,), 0, 4)
    flat_ids = jax.random.randint(key_flat, (TOKENS,), 0, EXPERTS)
    prim_exp = jnp.where(hot_coin == 0, hot_ids[hot_pick], flat_ids).astype(jnp.int32)
    alt_shift = jax.random.randint(key_alt, (TOKENS,), 1, EXPERTS)
    alt_exp = ((prim_exp + alt_shift) % EXPERTS).astype(jnp.int32)
    return prim_exp, alt_exp


def normal_mat(rand_key, arr_shape, mult_scale):
    return (jax.random.normal(rand_key, arr_shape, jnp.float32) * mult_scale).astype(jnp.bfloat16)


def setup_inputs(seed: int = 0, part: int = 0) -> dict:
    base_key = jax.random.key(seed)
    part_keys = jax.random.split(jax.random.fold_in(base_key, part), 3)
    weight_keys = jax.random.split(base_key, 7)
    prim_exp, alt_exp = draw_routes(part_keys[2])
    return dict(
        x_in=normal_mat(part_keys[0], (TOKENS, D), 1.0),
        y_grad=normal_mat(part_keys[1], (TOKENS, D), 1.0),
        prim_exp=prim_exp,
        alt_exp=alt_exp,
        w_router=normal_mat(weight_keys[0], (D, EXPERTS), D ** -0.5),
        exp_gate=normal_mat(weight_keys[1], (EXPERTS, D, FF), D ** -0.5),
        exp_up=normal_mat(weight_keys[2], (EXPERTS, D, FF), D ** -0.5),
        exp_down=normal_mat(weight_keys[3], (EXPERTS, FF, D), 0.5 * EXPERTS * FF ** -0.5),
        sh_gate=normal_mat(weight_keys[4], (D, FF), D ** -0.5),
        sh_up=normal_mat(weight_keys[5], (D, FF), D ** -0.5),
        sh_down=normal_mat(weight_keys[6], (FF, D), FF ** -0.5),
    )


def exclusive_rank(onehot):
    return jnp.sum((jnp.cumsum(onehot, axis=0) - onehot) * onehot, axis=1)


def route_tokens(prim_exp, alt_exp):
    expert_ids = jnp.arange(EXPERTS)
    one_prim = (prim_exp[:, None] == expert_ids[None, :]).astype(jnp.int32)
    rank_prim = exclusive_rank(one_prim)
    keep_prim = rank_prim < CAP
    kept_count = jnp.minimum(jnp.sum(one_prim, axis=0), CAP)
    overflow = jnp.logical_not(keep_prim).astype(jnp.int32)
    one_alt = (alt_exp[:, None] == expert_ids[None, :]).astype(jnp.int32) * overflow[:, None]
    slot_alt = exclusive_rank(one_alt) + jnp.sum(one_alt * kept_count[None, :], axis=1)
    keep_alt = (overflow == 1) & (slot_alt < CAP)
    assign = jnp.where(keep_prim, prim_exp, jnp.where(keep_alt, alt_exp, -1))
    slot_idx = jnp.where(keep_prim, rank_prim, slot_alt)
    return assign, slot_idx


def glu_forward(tok_rows, w_gate, w_up):
    act_gate = jnp.dot(tok_rows, w_gate, preferred_element_type=jnp.float32)
    act_up = jnp.dot(tok_rows, w_up, preferred_element_type=jnp.float32)
    hidden = (jax.nn.silu(act_gate) * act_up).astype(jnp.bfloat16)
    return hidden, act_gate, act_up


def glu_backward(d_hidden, act_gate, act_up):
    sig_gate = jax.nn.sigmoid(act_gate)
    d_gate = (d_hidden * act_up * sig_gate * (1.0 + act_gate * (1.0 - sig_gate))).astype(jnp.bfloat16)
    d_up = (d_hidden * act_gate * sig_gate).astype(jnp.bfloat16)
    return d_gate, d_up


def expert_forward(packed):
    tok_rows, w_gate, w_up, w_down = packed
    hidden, act_gate, act_up = glu_forward(tok_rows, w_gate, w_up)
    out_rows = jnp.dot(hidden, w_down, preferred_element_type=jnp.float32).astype(jnp.bfloat16)
    return hidden, act_gate, act_up, out_rows


def expert_backward(packed):
    tok_rows, d_rows, hidden, act_gate, act_up, w_gate, w_up, w_down = packed
    d_hidden = jnp.dot(d_rows, w_down.T, preferred_element_type=jnp.float32)
    g_down = jnp.dot(hidden.T, d_rows, preferred_element_type=jnp.float32)
    d_gate, d_up = glu_backward(d_hidden, act_gate, act_up)
    g_gate = jnp.dot(tok_rows.T, d_gate, preferred_element_type=jnp.float32)
    g_up = jnp.dot(tok_rows.T, d_up, preferred_element_type=jnp.float32)
    d_rows_in = (jnp.dot(d_gate, w_gate.T, preferred_element_type=jnp.float32) + jnp.dot(d_up, w_up.T, preferred_element_type=jnp.float32)).astype(jnp.bfloat16)
    return g_gate, g_up, g_down, d_rows_in


def reference(x_in, y_grad, prim_exp, alt_exp, w_router, exp_gate, exp_up, exp_down, sh_gate, sh_up, sh_down):
    x_wide = x_in.astype(jnp.float32)
    inv_rms = lax.rsqrt(jnp.mean(x_wide * x_wide, axis=1, keepdims=True) + EPS)
    normed = (x_wide * inv_rms).astype(jnp.bfloat16)
    gate_probs = jax.nn.softmax(jnp.dot(normed, w_router, preferred_element_type=jnp.float32), axis=1)
    assign, slot_idx = route_tokens(prim_exp, alt_exp)
    flat_pos = jnp.where(assign >= 0, assign * CAP + slot_idx, EXPERTS * CAP)
    slot_table = jnp.full((EXPERTS * CAP + 1,), TOKENS, jnp.int32).at[flat_pos].set(jnp.arange(TOKENS, dtype=jnp.int32))[: EXPERTS * CAP]
    expert_rows = jnp.take(normed, slot_table, axis=0, mode="fill", fill_value=0).reshape(EXPERTS, CAP, D)
    hidden, act_gate, act_up, out_rows = lax.map(expert_forward, (expert_rows, exp_gate, exp_up, exp_down))
    tok_out = jnp.take(out_rows.reshape(EXPERTS * CAP, D), flat_pos, axis=0, mode="fill", fill_value=0).astype(jnp.float32)
    one_assign = (assign[:, None] == jnp.arange(EXPERTS)[None, :]).astype(jnp.float32)
    gate_val = jnp.sum(gate_probs * one_assign, axis=1, keepdims=True)
    sh_hidden, sh_act_gate, sh_act_up = glu_forward(normed, sh_gate, sh_up)
    sh_out = jnp.dot(sh_hidden, sh_down, preferred_element_type=jnp.float32)
    y_out = (x_wide + sh_out + gate_val * tok_out).astype(jnp.bfloat16)
    dy_wide = y_grad.astype(jnp.float32)
    d_route = (gate_val * dy_wide).astype(jnp.bfloat16)
    d_gate_val = jnp.sum(dy_wide * tok_out, axis=1, keepdims=True)
    d_logits = (d_gate_val * gate_val * (one_assign - gate_probs)).astype(jnp.bfloat16)
    g_router = jnp.dot(normed.T, d_logits, preferred_element_type=jnp.float32)
    dn_router = jnp.dot(d_logits, w_router.T, preferred_element_type=jnp.float32)
    sh_d_hidden = jnp.dot(y_grad, sh_down.T, preferred_element_type=jnp.float32)
    g_sh_down = jnp.dot(sh_hidden.T, y_grad, preferred_element_type=jnp.float32)
    sh_d_gate, sh_d_up = glu_backward(sh_d_hidden, sh_act_gate, sh_act_up)
    g_sh_gate = jnp.dot(normed.T, sh_d_gate, preferred_element_type=jnp.float32)
    g_sh_up = jnp.dot(normed.T, sh_d_up, preferred_element_type=jnp.float32)
    dn_shared = jnp.dot(sh_d_gate, sh_gate.T, preferred_element_type=jnp.float32) + jnp.dot(sh_d_up, sh_up.T, preferred_element_type=jnp.float32)
    d_rows = jnp.take(d_route, slot_table, axis=0, mode="fill", fill_value=0).reshape(EXPERTS, CAP, D)
    g_exp_gate, g_exp_up, g_exp_down, d_rows_in = lax.map(expert_backward, (expert_rows, d_rows, hidden, act_gate, act_up, exp_gate, exp_up, exp_down))
    dn_routed = jnp.take(d_rows_in.reshape(EXPERTS * CAP, D), flat_pos, axis=0, mode="fill", fill_value=0).astype(jnp.float32)
    d_normed = dn_shared + dn_router + dn_routed
    norm_proj = jnp.mean(d_normed * x_wide, axis=1, keepdims=True)
    x_grad = (dy_wide + inv_rms * d_normed - x_wide * inv_rms ** 3 * norm_proj).astype(jnp.bfloat16)
    return (y_out, x_grad, g_exp_gate, g_exp_up, g_exp_down, g_sh_gate, g_sh_up, g_sh_down, g_router)
```

```python
import functools

import jax
import jax.numpy as jnp
from jax import lax
from jax.experimental import pallas as pl
from jax.experimental.pallas import tpu as pltpu
from jax.sharding import PartitionSpec as P

EPS = 1e-5
F32 = jnp.float32
BF16 = jnp.bfloat16
CHUNKS = 4
WIDTH_STEPS = 2


def glu_grads(d_hidden, act_gate, act_up):
    sig_gate = jax.nn.sigmoid(act_gate)
    d_gate = (d_hidden * act_up * sig_gate * (1.0 + act_gate * (1.0 - sig_gate))).astype(BF16)
    d_up = (d_hidden * act_gate * sig_gate).astype(BF16)
    return d_gate, d_up


def dot_nn(a, b):
    return lax.dot_general(a, b, (((1,), (0,)), ((), ())), preferred_element_type=F32)


def dot_nt(a, b):
    return lax.dot_general(a, b, (((1,), (1,)), ((), ())), preferred_element_type=F32)


def dot_tn(a, b):
    return lax.dot_general(a, b, (((0,), (0,)), ((), ())), preferred_element_type=F32)


def expert_kernel(n_alias, rank_ref, x_ref, u_ref, wg_ref, wu_ref, wd_ref, *rest):
    gwg_ref, gwu_ref, gwd_ref, keep_ref, send_ref, o_acc, dn_acc = rest[n_alias:]
    step = pl.program_id(1)
    last = pl.num_programs(1) - 1
    rows, cot = x_ref[0], u_ref[0]
    wg, wu, wd = wg_ref[0], wu_ref[0], wd_ref[0]
    act_gate = dot_nn(rows, wg)
    act_up = dot_nn(rows, wu)
    d_hidden = dot_nt(cot, wd)
    sig = jax.nn.sigmoid(act_gate)
    silu = act_gate * sig
    hidden = (silu * act_up).astype(BF16)
    d_gate = (d_hidden * act_up * sig * (1.0 + act_gate * (1.0 - sig))).astype(BF16)
    d_up = (d_hidden * silu).astype(BF16)
    o_part = dot_nn(hidden, wd)
    dn_part = dot_nt(d_gate, wg) + dot_nt(d_up, wu)
    gwd_ref[0] = dot_tn(hidden, cot)
    gwg_ref[0] = dot_tn(rows, d_gate)
    gwu_ref[0] = dot_tn(rows, d_up)

    @pl.when(step == 0)
    def _():
        o_acc[...] = o_part
        dn_acc[...] = dn_part

    @pl.when(step > 0)
    def _():
        o_acc[...] += o_part
        dn_acc[...] += dn_part

    half = o_acc.shape[1] // 2

    @pl.when((step == last) & (rank_ref[0] == 0))
    def _():
        keep_ref[:, :half] = o_acc[:, :half]
        keep_ref[:, half:] = dn_acc[:, :half]
        send_ref[:, :half] = o_acc[:, half:]
        send_ref[:, half:] = dn_acc[:, half:]

    @pl.when((step == last) & (rank_ref[0] == 1))
    def _():
        keep_ref[:, :half] = o_acc[:, half:]
        keep_ref[:, half:] = dn_acc[:, half:]
        send_ref[:, :half] = o_acc[:, :half]
        send_ref[:, half:] = dn_acc[:, :half]


def expert_chunk(first, count, rank, rows, cot, wg, wu, wd, grads):
    num, dim, width = wg.shape
    cap = rows.shape[1]
    tile = width // WIDTH_STEPS
    any_spec = pl.BlockSpec(memory_space=pl.ANY)
    row_spec = pl.BlockSpec((1, cap, dim), lambda e, f: (first + e, 0, 0))
    in_spec = pl.BlockSpec((1, dim, tile), lambda e, f: (first + e, 0, f))
    down_spec = pl.BlockSpec((1, tile, dim), lambda e, f: (first + e, f, 0))
    out_rows = pl.BlockSpec((cap, dim), lambda e, f: (e, 0))
    n_alias = len(grads)
    flops = 9 * 2 * count * cap * dim * width
    nbytes = count * 3 * dim * width * 6
    return pl.pallas_call(
        functools.partial(expert_kernel, n_alias),
        grid=(count, WIDTH_STEPS),
        in_specs=[pl.BlockSpec(memory_space=pltpu.SMEM), row_spec, row_spec, in_spec, in_spec, down_spec] + [any_spec] * n_alias,
        out_specs=[in_spec, in_spec, down_spec, out_rows, out_rows],
        out_shape=[
            jax.ShapeDtypeStruct((num, dim, width), F32),
            jax.ShapeDtypeStruct((num, dim, width), F32),
            jax.ShapeDtypeStruct((num, width, dim), F32),
            jax.ShapeDtypeStruct((count * cap, dim), F32),
            jax.ShapeDtypeStruct((count * cap, dim), F32),
        ],
        scratch_shapes=[pltpu.VMEM((cap, dim), F32), pltpu.VMEM((cap, dim), F32)],
        input_output_aliases={6 + i: i for i in range(n_alias)},
        compiler_params=pltpu.CompilerParams(dimension_semantics=("arbitrary", "arbitrary"), vmem_limit_bytes=56 * 1024 * 1024),
        cost_estimate=pl.CostEstimate(flops=flops, bytes_accessed=nbytes, transcendentals=0),
        name="experts",
    )(rank, rows, cot, wg, wu, wd, *grads)


def exclusive_rank(onehot):
    num, tokens = onehot.shape
    blk = 256
    nb = tokens // blk
    below = (jnp.arange(blk)[:, None] < jnp.arange(blk)[None, :]).astype(BF16)
    parts = onehot.reshape(num * nb, blk)
    local = dot_nn(parts, below).reshape(num, nb, blk)
    sums = jnp.sum(parts.astype(F32), axis=1).reshape(num, nb)
    earlier = (jnp.arange(nb)[:, None] < jnp.arange(nb)[None, :]).astype(F32)
    base = jnp.sum(sums[:, :, None] * earlier[None], axis=1)
    ranks = (local + base[:, :, None]).reshape(num, tokens)
    rank = jnp.sum(ranks * onehot.astype(F32), axis=0)
    return rank, jnp.sum(sums, axis=1)


def solution(mesh):
    ep_size = mesh.shape["ep"]
    tok_spec = P(("dp", "ep"), None)
    id_spec = P(("dp", "ep"))
    in_specs = (tok_spec, tok_spec, id_spec, id_spec, P(None, None), P("ep", None, "etp"), P("ep", None, "etp"), P("ep", "etp", None), P(None, "etp"), P(None, "etp"), P("etp", None))
    out_specs = (tok_spec, tok_spec, P(("dp", "ep"), None, "etp"), P(("dp", "ep"), None, "etp"), P(("dp", "ep"), "etp", None), P("dp", "etp"), P("dp", "etp"), P(("dp", "etp"), None), P("dp", None))
    swap_x = lambda v: lax.ppermute(v, "ep", [(i, i ^ 2) for i in range(ep_size)])
    swap_c = lambda v: lax.ppermute(v, "ep", [(i, i ^ 1) for i in range(ep_size)])
    swap_y = lambda v: lax.ppermute(v, "etp", [(0, 1), (1, 0)])

    def spread(v):
        far = swap_x(v)
        return [v, swap_c(v), far, swap_c(far)]

    def local_step(x_in, y_grad, prim_exp, alt_exp, w_router, exp_gate, exp_up, exp_down, sh_gate, sh_up, sh_down):
        tok_local, model_dim = x_in.shape
        num_exp = w_router.shape[1]
        local_exp = exp_gate.shape[0]
        capacity = 5 * tok_local * ep_size // (4 * num_exp)
        local_slots = local_exp * capacity
        half = model_dim // 2
        rank = lax.axis_index("ep")
        etp = lax.axis_index("etp")
        my_col, other_col = etp * half, (1 - etp) * half
        cols = lambda v: lax.dynamic_slice_in_dim(v, my_col, half, 1)

        x_wide = x_in.astype(F32)
        inv_rms = lax.rsqrt(jnp.mean(x_wide * x_wide, axis=1, keepdims=True) + EPS)
        normed = (x_wide * inv_rms).astype(BF16)
        ids = spread(jnp.stack([prim_exp, alt_exp]))
        n_blocks = spread(normed)
        dy_blocks = spread(y_grad)

        sh_act_gate = dot_nn(normed, sh_gate)
        sh_act_up = dot_nn(normed, sh_up)
        sh_hidden = (jax.nn.silu(sh_act_gate) * sh_act_up).astype(BF16)
        down_keep = lax.dynamic_slice_in_dim(sh_down, my_col, half, 1)
        down_send = lax.dynamic_slice_in_dim(sh_down, other_col, half, 1)
        sh_recv = swap_y(dot_nn(sh_hidden, down_send))
        sh_out = dot_nn(sh_hidden, down_keep) + sh_recv
        sh_d_gate, sh_d_up = glu_grads(dot_nt(y_grad, sh_down), sh_act_gate, sh_act_up)

        def shared_dn(col):
            return dot_nt(sh_d_gate, lax.dynamic_slice_in_dim(sh_gate, col, half, 0)) + dot_nt(sh_d_up, lax.dynamic_slice_in_dim(sh_up, col, half, 0))

        dn_recv = swap_y(shared_dn(other_col))
        dn_shared = shared_dn(my_col) + dn_recv

        ids_all = jnp.take(jnp.stack(ids), rank ^ jnp.arange(ep_size), axis=0)
        prim_all = ids_all[:, 0, :].reshape(1, -1)
        alt_all = ids_all[:, 1, :].reshape(1, -1)
        expert_col = jnp.arange(num_exp)[:, None]
        one_prim = (prim_all == expert_col).astype(BF16)
        rank_prim, prim_counts = exclusive_rank(one_prim)
        keep_prim = rank_prim < capacity
        kept = jnp.minimum(prim_counts, float(capacity))
        one_alt = ((alt_all == expert_col) & jnp.logical_not(keep_prim)[None, :]).astype(BF16)
        rank_alt, _ = exclusive_rank(one_alt)
        slot_alt = rank_alt + jnp.sum(one_alt.astype(F32) * kept[:, None], axis=0)
        keep_alt = jnp.logical_not(keep_prim) & (slot_alt < capacity)
        assign = jnp.where(keep_prim, prim_all[0], jnp.where(keep_alt, alt_all[0], num_exp))
        slot = jnp.where(keep_prim, rank_prim, jnp.where(keep_alt, slot_alt, 0.0)).astype(jnp.int32)
        pos = (assign * capacity + slot).reshape(ep_size, tok_local)
        pos_blocks = jnp.take(pos, rank ^ jnp.arange(ep_size), axis=0)
        pos_own = pos_blocks[0]
        assign_own = lax.dynamic_slice_in_dim(assign.reshape(ep_size, tok_local), rank, 1, 0).reshape(tok_local, 1)

        gate_probs = jax.nn.softmax(dot_nn(normed, w_router), axis=1)
        one_assign = (assign_own == jnp.arange(num_exp)[None, :]).astype(F32)
        gate_val = jnp.sum(gate_probs * one_assign, axis=1, keepdims=True)
        g_all = jnp.concatenate(spread(gate_val.reshape(1, tok_local)), axis=1)

        target = pos_blocks.reshape(1, -1) - rank * local_slots
        slot_col = jnp.arange(local_slots)[:, None]
        n_all = jnp.concatenate(n_blocks, axis=0)
        dy_all = jnp.concatenate(dy_blocks, axis=0)
        pick = target == slot_col
        rows = dot_nn(pick.astype(BF16), n_all).astype(BF16).reshape(local_exp, capacity, model_dim)
        g_slot = jnp.sum(jnp.where(pick, g_all, 0.0), axis=1, keepdims=True)
        cot = (g_slot * dot_nn(pick.astype(BF16), dy_all)).astype(BF16).reshape(local_exp, capacity, model_dim)

        per = local_exp // CHUNKS
        rank_arr = etp.reshape(1).astype(jnp.int32)
        grads = ()
        picked = jnp.zeros((tok_local, model_dim), F32)
        pos_col = pos_own.reshape(tok_local, 1)
        for c in range(CHUNKS):
            gwg, gwu, gwd, keep, send = expert_chunk(c * per, per, rank_arr, rows, cot, exp_gate, exp_up, exp_down, grads)
            grads = (gwg, gwu, gwd)
            final = (keep + swap_y(send)).astype(BF16)
            blocks = jnp.concatenate(spread(final), axis=0)
            owner = rank ^ jnp.arange(ep_size)
            ids_row = (owner[:, None] * local_slots + c * per * capacity + jnp.arange(per * capacity)[None, :]).reshape(1, -1)
            picked = picked + dot_nn((pos_col == ids_row).astype(BF16), blocks)
        tok_out, dn_routed = picked[:, :half], picked[:, half:]

        x_half, dy_half = cols(x_in).astype(F32), cols(y_grad).astype(F32)
        y_half = (x_half + sh_out + gate_val * tok_out).astype(BF16)
        dg_part = jnp.sum(dy_half * tok_out, axis=1).reshape(1, tok_local)
        d_gate_val = (dg_part + swap_y(dg_part)).reshape(tok_local, 1)
        d_logits = (d_gate_val * gate_val * (one_assign - gate_probs)).astype(BF16)
        router_part = dot_tn(d_logits, normed)
        router_part = router_part + swap_c(router_part)
        g_router = (router_part + swap_x(router_part)).T
        dn_router = dot_nt(d_logits, lax.dynamic_slice_in_dim(w_router, my_col, half, 0))
        d_normed = dn_shared + dn_router + dn_routed
        proj_part = jnp.sum(d_normed * x_half, axis=1).reshape(1, tok_local)
        norm_proj = ((proj_part + swap_y(proj_part)) / model_dim).reshape(tok_local, 1)
        xg_half = (dy_half + inv_rms * d_normed - x_half * inv_rms ** 3 * norm_proj).astype(BF16)

        def whole_cols(mine):
            other = swap_y(mine)
            return jnp.where(etp == 0, jnp.concatenate([mine, other], 1), jnp.concatenate([other, mine], 1))

        y_out = whole_cols(y_half)
        x_grad = whole_cols(xg_half)

        core = rank % 2
        tile = sh_gate.shape[1] // 2
        w_gate = lax.dynamic_slice_in_dim(sh_gate, core * tile, tile, 1)
        w_up = lax.dynamic_slice_in_dim(sh_up, core * tile, tile, 1)
        w_down = lax.dynamic_slice_in_dim(sh_down, core * tile, tile, 0)
        all_gate = dot_nn(n_all, w_gate)
        all_up = dot_nn(n_all, w_up)
        all_hidden = (jax.nn.silu(all_gate) * all_up).astype(BF16)
        all_d_gate, all_d_up = glu_grads(dot_nt(dy_all, w_down), all_gate, all_up)

        def whole_width(mine, axis):
            other = swap_c(mine)
            return jnp.where(core == 0, jnp.concatenate([mine, other], axis), jnp.concatenate([other, mine], axis))

        g_sh_gate = whole_width(dot_tn(n_all, all_d_gate), 1)
        g_sh_up = whole_width(dot_tn(n_all, all_d_up), 1)
        g_sh_down = whole_width(dot_tn(all_hidden, dy_all), 0)
        return (y_out, x_grad, *grads, g_sh_gate, g_sh_up, g_sh_down, g_router)

    return jax.shard_map(local_step, mesh=mesh, in_specs=in_specs, out_specs=out_specs, check_vma=False)
```

```python
import functools

import jax
import jax.numpy as jnp
from jax import lax
from jax.experimental import pallas as pl
from jax.experimental.pallas import tpu as pltpu
from jax.sharding import PartitionSpec as P


EPS = 1e-5
F32 = jnp.float32
BF16 = jnp.bfloat16
SPLIT = (3, 3, 2)
WIDTH_STEPS = 2
TOKEN_TILE = 512
TOKEN_PARTS = 2
PICK_STEPS = 4


def glu_parts(d_hidden, act_gate, act_up):
    sig = 0.5 * jnp.tanh(0.5 * act_gate) + 0.5
    silu = act_gate * sig
    hidden = (silu * act_up).astype(BF16)
    d_gate = (d_hidden * act_up * (sig + silu * (1.0 - sig))).astype(BF16)
    return hidden, d_gate, (d_hidden * silu).astype(BF16)


def dot_nn(a, b):
    return lax.dot_general(a, b, (((1,), (0,)), ((), ())), preferred_element_type=F32)


def dot_nt(a, b):
    return lax.dot_general(a, b, (((1,), (1,)), ((), ())), preferred_element_type=F32)


def dot_tn(a, b):
    return lax.dot_general(a, b, (((0,), (0,)), ((), ())), preferred_element_type=F32)


def expert_kernel(n_alias, rank_ref, x_ref, u_ref, wg_ref, wu_ref, wd_ref, *rest):
    gwg_ref, gwu_ref, gwd_ref, keep_ref, send_ref, o_acc, dn_acc = rest[n_alias:]
    step = pl.program_id(1)
    last = pl.num_programs(1) - 1
    rows, cot = x_ref[0], u_ref[0]
    wg, wu, wd = wg_ref[0], wu_ref[0], wd_ref[0]
    act_gate = dot_nn(rows, wg)
    act_up = dot_nn(rows, wu)
    d_hidden = dot_nt(cot, wd)
    hidden, d_gate, d_up = glu_parts(d_hidden, act_gate, act_up)
    o_part = dot_nn(hidden, wd)
    dn_part = dot_nt(d_gate, wg) + dot_nt(d_up, wu)
    gwd_ref[0] = dot_tn(hidden, cot)
    gwg_ref[0] = dot_tn(rows, d_gate)
    gwu_ref[0] = dot_tn(rows, d_up)

    @pl.when(step == 0)
    def _():
        o_acc[...] = o_part
        dn_acc[...] = dn_part

    @pl.when(step > 0)
    def _():
        o_acc[...] += o_part
        dn_acc[...] += dn_part

    half = o_acc.shape[1] // 2

    @pl.when((step == last) & (rank_ref[0] == 0))
    def _():
        keep_ref[:, :half] = o_acc[:, :half]
        keep_ref[:, half:] = dn_acc[:, :half]
        send_ref[:, :half] = o_acc[:, half:]
        send_ref[:, half:] = dn_acc[:, half:]

    @pl.when((step == last) & (rank_ref[0] == 1))
    def _():
        keep_ref[:, :half] = o_acc[:, half:]
        keep_ref[:, half:] = dn_acc[:, half:]
        send_ref[:, :half] = o_acc[:, :half]
        send_ref[:, half:] = dn_acc[:, :half]


def expert_chunk(first, count, rank, rows, cot, wg, wu, wd, grads):
    num, dim, width = wg.shape
    cap = rows.shape[1]
    tile = width // WIDTH_STEPS
    any_spec = pl.BlockSpec(memory_space=pl.ANY)
    row_spec = pl.BlockSpec((1, cap, dim), lambda e, f: (first + e, 0, 0))
    in_spec = pl.BlockSpec((1, dim, tile), lambda e, f: (first + e, 0, f))
    down_spec = pl.BlockSpec((1, tile, dim), lambda e, f: (first + e, f, 0))
    out_rows = pl.BlockSpec((cap, dim), lambda e, f: (e, 0))
    n_alias = len(grads)
    flops = 9 * 2 * count * cap * dim * width
    nbytes = count * 3 * dim * width * 6
    return pl.pallas_call(
        functools.partial(expert_kernel, n_alias),
        grid=(count, WIDTH_STEPS),
        in_specs=[pl.BlockSpec(memory_space=pltpu.SMEM), row_spec, row_spec, in_spec, in_spec, down_spec] + [any_spec] * n_alias,
        out_specs=[in_spec, in_spec, down_spec, out_rows, out_rows],
        out_shape=[
            jax.ShapeDtypeStruct((num, dim, width), F32),
            jax.ShapeDtypeStruct((num, dim, width), F32),
            jax.ShapeDtypeStruct((num, width, dim), F32),
            jax.ShapeDtypeStruct((count * cap, dim), F32),
            jax.ShapeDtypeStruct((count * cap, dim), F32),
        ],
        scratch_shapes=[pltpu.VMEM((cap, dim), F32), pltpu.VMEM((cap, dim), F32)],
        input_output_aliases={6 + i: i for i in range(n_alias)},
        compiler_params=pltpu.CompilerParams(dimension_semantics=("arbitrary", "arbitrary"), vmem_limit_bytes=56 * 1024 * 1024),
        cost_estimate=pl.CostEstimate(flops=flops, bytes_accessed=nbytes, transcendentals=0),
        name="experts",
    )(rank, rows, cot, wg, wu, wd, *grads)


def shared_kernel(mode, ids_ref, n_a, n_b, dy_a, dy_b, wg_ref, wu_ref, wd_ref, *rest):
    first_half = pl.program_id(0) == 0
    start = first_half & (pl.program_id(1) == 0)
    if mode == 0:
        hg_ref, hu_ref, hd_ref, mine_ref, other_ref, gg_ref, gu_ref, gd_ref = rest
    elif mode == 1:
        hg_ref, hu_ref, hd_ref, mine_in, other_in, mine_ref, other_ref = rest
    else:
        pg_ref, pu_ref, pd_ref, gg_ref, gu_ref, gd_ref, fg_ref, fu_ref, fd_ref = rest
    rows = jnp.where(first_half, n_a[...], n_b[...])
    cot = jnp.where(first_half, dy_a[...], dy_b[...])
    wg, wu, wd = wg_ref[...], wu_ref[...], wd_ref[...]
    part = rows.shape[0] // TOKEN_PARTS
    acts = []
    for i in range(TOKEN_PARTS):
        own, own_cot = rows[i * part : (i + 1) * part], cot[i * part : (i + 1) * part]
        acts.append((dot_nt(own_cot, wd), dot_nn(own, wg), dot_nn(own, wu)))
    hidden, d_gate, d_up = [jnp.concatenate(v, axis=0) for v in zip(*[glu_parts(*v) for v in acts])]
    if mode != 1:
        @pl.when(start)
        def _():
            gg_ref[...] = pg_ref[...] if mode else jnp.zeros_like(gg_ref)
            gu_ref[...] = pu_ref[...] if mode else jnp.zeros_like(gu_ref)
            gd_ref[...] = pd_ref[...] if mode else jnp.zeros_like(gd_ref)

        gg_ref[...] += dot_tn(rows, d_gate)
        gu_ref[...] += dot_tn(rows, d_up)
        gd_ref[...] += dot_tn(hidden, cot)
    if mode != 2:
        half = hd_ref.shape[1]
        out = dot_nn(hidden, hd_ref[...])
        dn = dot_nt(d_gate, hg_ref[...]) + dot_nt(d_up, hu_ref[...])

        @pl.when(first_half)
        def _():
            mine_ref[:, :half] = out + mine_in[:, :half] if mode else out
            mine_ref[:, half:] = dn + mine_in[:, half:] if mode else dn

        @pl.when(jnp.logical_not(first_half))
        def _():
            other_ref[:, :half] = out + other_in[:, :half] if mode else out
            other_ref[:, half:] = dn + other_in[:, half:] if mode else dn
    else:
        @pl.when(jnp.logical_not(first_half) & (pl.program_id(1) == pl.num_programs(1) - 1))
        def _():
            fg_ref[...] = gg_ref[...]
            fu_ref[...] = gu_ref[...]
            fd_ref[...] = gd_ref[...]


def shared_pass(mode, ids, n_pair, dy_pair, weights, earlier=()):
    tokens, dim = n_pair[0].shape
    tok, half = TOKEN_TILE, dim // 2
    tile = weights[0].shape[1] // (1 if mode == 1 else 2)
    steps = tokens // tok
    one = pl.Buffered(1)
    part = (lambda ids: 0) if mode == 1 else (lambda ids: ids[0])
    early = lambda w: pl.BlockSpec((tok, w), lambda h, j, ids: (jnp.where(h == 0, j, steps - 1), 0))
    late = lambda w: pl.BlockSpec((tok, w), lambda h, j, ids: (jnp.where(h == 0, 0, j), 0))
    col = pl.BlockSpec((dim, tile), lambda h, j, ids: (0, part(ids)), pipeline_mode=one)
    row = pl.BlockSpec((tile, dim), lambda h, j, ids: (part(ids), 0), pipeline_mode=one)
    half_row = pl.BlockSpec((half, tile), lambda h, j, ids: (ids[1], part(ids)), pipeline_mode=one)
    half_col = pl.BlockSpec((tile, half), lambda h, j, ids: (part(ids), ids[1]), pipeline_mode=one)
    sums = [(dim, tile), (dim, tile), (tile, dim)]
    sum_specs = [pl.BlockSpec(v, lambda h, j, ids: (0, 0), pipeline_mode=one) for v in sums]
    sum_shapes = [jax.ShapeDtypeStruct(v, F32) for v in sums]
    row_specs = [early(dim), late(dim)]
    row_shapes = [jax.ShapeDtypeStruct((tokens, dim), F32)] * 2
    in_specs = [early(dim), late(dim), early(dim), late(dim), col, col, row]
    args = [*n_pair, *dy_pair, *weights]
    if mode != 2:
        in_specs += [half_row, half_row, half_col]
        args += list(weights)
    if mode == 1:
        in_specs += row_specs
    if mode == 2:
        in_specs += sum_specs
    args += list(earlier)
    if mode == 0:
        out_specs, out_shape = row_specs + sum_specs, row_shapes + sum_shapes
    elif mode == 1:
        out_specs, out_shape = row_specs, row_shapes
    else:
        width = 2 * tile
        out_specs = sum_specs + [col, col, row]
        out_shape = sum_shapes + [jax.ShapeDtypeStruct(v, F32) for v in ((dim, width), (dim, width), (width, dim))]
    dots = (7.5, 4.5, 6)[mode]
    return pl.pallas_call(
        functools.partial(shared_kernel, mode),
        grid_spec=pltpu.PrefetchScalarGridSpec(num_scalar_prefetch=1, grid=(2, steps), in_specs=in_specs, out_specs=out_specs),
        out_shape=out_shape,
        compiler_params=pltpu.CompilerParams(dimension_semantics=("arbitrary", "arbitrary"), vmem_limit_bytes=60 * 1024 * 1024),
        cost_estimate=pl.CostEstimate(flops=int(dots * 4 * tokens * dim * tile), bytes_accessed=30 * 1024 * 1024, transcendentals=0),
    )(ids, *args)


def place_kernel(core_ref, a_ref, b_ref, c_ref, ah, bh, ch, ao_ref, bo_ref, co_ref):
    ao_ref[...] = a_ref[...]
    bo_ref[...] = b_ref[...]
    co_ref[...] = c_ref[...]


def place_halves(core, parts, whole):
    dim, tile = parts[0].shape
    steps = 4
    any_spec = pl.BlockSpec(memory_space=pl.ANY)
    in_row = pl.BlockSpec((dim // steps, tile), lambda j, core: (j, 0))
    down_row = pl.BlockSpec((tile // steps, dim), lambda j, core: (j, 0))
    out_col = pl.BlockSpec((dim // steps, tile), lambda j, core: (j, 1 - core[0]))
    out_row = pl.BlockSpec((tile // steps, dim), lambda j, core: ((1 - core[0]) * steps + j, 0))
    return pl.pallas_call(
        place_kernel,
        grid_spec=pltpu.PrefetchScalarGridSpec(num_scalar_prefetch=1, grid=(steps,), in_specs=[in_row, in_row, down_row] + [any_spec] * 3, out_specs=[out_col, out_col, out_row]),
        out_shape=[jax.ShapeDtypeStruct(w.shape, F32) for w in whole],
        input_output_aliases={4: 0, 5: 1, 6: 2},
        cost_estimate=pl.CostEstimate(flops=1000000, bytes_accessed=15 * 1024 * 1024, transcendentals=0),
        name="place",
    )(core, *parts, *whole)


def pick_kernel(tgt_ref, *refs):
    srcs, out = refs[:-1], refs[-1]
    tok = srcs[0].shape[0]
    slot = lax.broadcasted_iota(jnp.int32, (out.shape[0], tok), 0) + pl.program_id(0) * out.shape[0]
    got = None
    for i, src in enumerate(srcs):
        term = dot_nn((tgt_ref[:, i * tok : (i + 1) * tok] == slot).astype(BF16), src[...])
        got = term if got is None else got + term
    out[...] = got.astype(BF16)


def pick_rows(target, blocks, slots):
    tok, dim = blocks[0].shape
    tile = slots // PICK_STEPS
    whole = pl.BlockSpec((tok, dim), lambda e: (0, 0), pipeline_mode=pl.Buffered(1))
    return pl.pallas_call(
        pick_kernel,
        grid=(PICK_STEPS,),
        in_specs=[pl.BlockSpec((1, len(blocks) * tok), lambda e: (0, 0))] + [whole] * len(blocks),
        out_specs=pl.BlockSpec((tile, dim), lambda e: (e, 0)),
        out_shape=jax.ShapeDtypeStruct((slots, dim), BF16),
        compiler_params=pltpu.CompilerParams(dimension_semantics=("arbitrary",), vmem_limit_bytes=48 * 1024 * 1024),
        cost_estimate=pl.CostEstimate(flops=2 * slots * len(blocks) * tok * dim, bytes_accessed=8 * 1024 * 1024, transcendentals=0),
        name="pick",
    )(target, *blocks)


def join_kernel(etp_ref, *refs):
    n = len(refs) // 3
    for i in range(n):
        mine, other, out = refs[2 * i], refs[2 * i + 1], refs[2 * n + i]
        half = mine.shape[1]

        @pl.when(etp_ref[0] == 0)
        def _():
            out[:, :half] = mine[...]
            out[:, half:] = other[...]

        @pl.when(etp_ref[0] == 1)
        def _():
            out[:, :half] = other[...]
            out[:, half:] = mine[...]


def join_cols(etp, pairs):
    tokens, half = pairs[0][0].shape
    tok = tokens // 2
    spec = pl.BlockSpec((tok, half), lambda j: (j, 0))
    return pl.pallas_call(
        join_kernel,
        grid=(2,),
        in_specs=[pl.BlockSpec(memory_space=pltpu.SMEM)] + [spec] * (2 * len(pairs)),
        out_specs=[pl.BlockSpec((tok, 2 * half), lambda j: (j, 0))] * len(pairs),
        out_shape=[jax.ShapeDtypeStruct((tokens, 2 * half), BF16)] * len(pairs),
        cost_estimate=pl.CostEstimate(flops=1000000, bytes_accessed=6 * 1024 * 1024, transcendentals=0),
        name="join",
    )(etp, *[v for p in pairs for v in p])


def exclusive_rank(onehot):
    num, tokens = onehot.shape
    blk = 256
    nb = tokens // blk
    below = (jnp.arange(blk)[:, None] < jnp.arange(blk)[None, :]).astype(BF16)
    parts = onehot.reshape(num * nb, blk)
    local = dot_nn(parts, below).reshape(num, nb, blk)
    sums = jnp.sum(parts.astype(F32), axis=1).reshape(num, nb)
    earlier = (jnp.arange(nb)[:, None] < jnp.arange(nb)[None, :]).astype(F32)
    base = jnp.sum(sums[:, :, None] * earlier[None], axis=1)
    ranks = (local + base[:, :, None]).reshape(num, tokens)
    rank = jnp.sum(ranks * onehot.astype(F32), axis=0)
    return rank, jnp.sum(sums, axis=1)


def solution(mesh):
    ep_size = mesh.shape["ep"]
    tok_spec = P(("dp", "ep"), None)
    id_spec = P(("dp", "ep"))
    in_specs = (tok_spec, tok_spec, id_spec, id_spec, P(None, None), P("ep", None, "etp"), P("ep", None, "etp"), P("ep", "etp", None), P(None, "etp"), P(None, "etp"), P("etp", None))
    out_specs = (tok_spec, tok_spec, P(("dp", "ep"), None, "etp"), P(("dp", "ep"), None, "etp"), P(("dp", "ep"), "etp", None), P("dp", "etp"), P("dp", "etp"), P(("dp", "etp"), None), P("dp", None))
    swap_x = lambda v: lax.ppermute(v, "ep", [(i, i ^ 2) for i in range(ep_size)])
    swap_c = lambda v: lax.ppermute(v, "ep", [(i, i ^ 1) for i in range(ep_size)])
    swap_y = lambda v: lax.ppermute(v, "etp", [(0, 1), (1, 0)])

    def spread(v):
        far = swap_x(v)
        return [v, swap_c(v), far, swap_c(far)]

    def local_work(x_in, y_grad, prim_exp, alt_exp, w_router, exp_gate, exp_up, exp_down, sh_gate, sh_up, sh_down):
        tok_local, model_dim = x_in.shape
        num_exp = w_router.shape[1]
        local_exp = exp_gate.shape[0]
        capacity = 5 * tok_local * ep_size // (4 * num_exp)
        local_slots = local_exp * capacity
        half = model_dim // 2
        rank = lax.axis_index("ep")
        etp = lax.axis_index("etp")
        my_col = etp * half
        cols = lambda v: lax.dynamic_slice_in_dim(v, my_col, half, 1)

        x_wide = x_in.astype(F32)
        inv_rms = lax.rsqrt(jnp.mean(x_wide * x_wide, axis=1, keepdims=True) + EPS)
        normed = (x_wide * inv_rms).astype(BF16)
        ids = spread(jnp.stack([prim_exp, alt_exp]))
        dy_blocks = spread(y_grad)
        n_blocks = spread(normed)

        core = rank % 2
        ids_arr = jnp.stack([core, etp]).astype(jnp.int32)
        etp_arr = ids_arr[1:]
        tile = sh_gate.shape[1] // 2
        part = lambda v, axis: lax.dynamic_slice_in_dim(v, core * tile, tile, axis)
        far_weights = [swap_y(part(v, axis)) for v, axis in ((sh_gate, 1), (sh_up, 1), (sh_down, 0))]
        sh_mine, sh_other, *sh_sums = shared_pass(0, ids_arr, n_blocks[:2], dy_blocks[:2], (sh_gate, sh_up, sh_down))
        sh_mine, sh_other = shared_pass(1, ids_arr, n_blocks[:2], dy_blocks[:2], far_weights, (sh_mine, sh_other))
        sh_half = sh_mine + swap_c(sh_other)
        sh_out, dn_shared = sh_half[:, :half], sh_half[:, half:]

        ids_all = jnp.take(jnp.stack(ids), rank ^ jnp.arange(ep_size), axis=0)
        prim_all = ids_all[:, 0, :].reshape(1, -1)
        alt_all = ids_all[:, 1, :].reshape(1, -1)
        expert_col = jnp.arange(num_exp)[:, None]
        one_prim = (prim_all == expert_col).astype(BF16)
        rank_prim, prim_counts = exclusive_rank(one_prim)
        keep_prim = rank_prim < capacity
        kept = jnp.minimum(prim_counts, float(capacity))
        one_alt = ((alt_all == expert_col) & jnp.logical_not(keep_prim)[None, :]).astype(BF16)
        rank_alt, _ = exclusive_rank(one_alt)
        slot_alt = rank_alt + jnp.sum(one_alt.astype(F32) * kept[:, None], axis=0)
        keep_alt = jnp.logical_not(keep_prim) & (slot_alt < capacity)
        assign = jnp.where(keep_prim, prim_all[0], jnp.where(keep_alt, alt_all[0], num_exp))
        slot = jnp.where(keep_prim, rank_prim, jnp.where(keep_alt, slot_alt, 0.0)).astype(jnp.int32)
        pos = (assign * capacity + slot).reshape(ep_size, tok_local)
        pos_blocks = jnp.take(pos, rank ^ jnp.arange(ep_size), axis=0)
        pos_own = pos_blocks[0]
        assign_own = lax.dynamic_slice_in_dim(assign.reshape(ep_size, tok_local), rank, 1, 0).reshape(tok_local, 1)

        gate_probs = jax.nn.softmax(dot_nn(normed, w_router), axis=1)
        one_assign = (assign_own == jnp.arange(num_exp)[None, :]).astype(F32)
        gate_val = jnp.sum(gate_probs * one_assign, axis=1, keepdims=True)

        target = pos_blocks.reshape(1, -1) - rank * local_slots
        rows = pick_rows(target, n_blocks, local_slots)
        slot_probs = jax.nn.softmax(dot_nn(rows, w_router), axis=1)
        slot_expert = rank * local_exp + jnp.arange(local_slots)[:, None] // capacity
        g_slot = jnp.sum(jnp.where(slot_expert == jnp.arange(num_exp)[None, :], slot_probs, 0.0), axis=1, keepdims=True)
        dy_rows = pick_rows(target, dy_blocks, local_slots)
        rows = rows.reshape(local_exp, capacity, model_dim)
        cot = (g_slot * dy_rows.astype(F32)).astype(BF16).reshape(local_exp, capacity, model_dim)

        grads = ()
        picked = jnp.zeros((tok_local, model_dim), F32)
        pos_col = pos_own.reshape(tok_local, 1)
        first = 0
        for per in SPLIT:
            gwg, gwu, gwd, keep, send = expert_chunk(first, per, etp_arr, rows, cot, exp_gate, exp_up, exp_down, grads)
            grads = (gwg, gwu, gwd)
            final = (keep + swap_y(send)).astype(BF16)
            blocks = jnp.concatenate(spread(final), axis=0)
            owner = rank ^ jnp.arange(ep_size)
            ids_row = (owner[:, None] * local_slots + first * capacity + jnp.arange(per * capacity)[None, :]).reshape(1, -1)
            picked = picked + dot_nn((pos_col == ids_row).astype(BF16), blocks)
            first += per
        tok_out, dn_routed = picked[:, :half], picked[:, half:]

        x_half, dy_half = cols(x_in).astype(F32), cols(y_grad).astype(F32)
        y_half = (x_half + sh_out + gate_val * tok_out).astype(BF16)
        dg_part = jnp.sum(dy_half * tok_out, axis=1).reshape(1, tok_local)
        d_gate_val = (dg_part + swap_y(dg_part)).reshape(tok_local, 1)
        d_logits = (d_gate_val * gate_val * (one_assign - gate_probs)).astype(BF16)
        router_part = dot_tn(d_logits, normed)
        router_part = router_part + swap_c(router_part)
        g_router = (router_part + swap_x(router_part)).T
        dn_router = dot_nt(d_logits, lax.dynamic_slice_in_dim(w_router, my_col, half, 0))
        d_normed = dn_shared + dn_router + dn_routed
        proj_part = jnp.sum(d_normed * x_half, axis=1).reshape(1, tok_local)
        norm_proj = ((proj_part + swap_y(proj_part)) / model_dim).reshape(tok_local, 1)
        xg_half = (dy_half + inv_rms * d_normed - x_half * inv_rms ** 3 * norm_proj).astype(BF16)

        y_recv = swap_y(y_half)
        xg_recv = swap_y(xg_half)
        y_out, x_grad = join_cols(etp_arr, [(y_half, y_recv), (xg_half, xg_recv)])

        out = shared_pass(2, ids_arr, n_blocks[2:], dy_blocks[2:], (sh_gate, sh_up, sh_down), sh_sums)
        g_sh_gate, g_sh_up, g_sh_down = place_halves(ids_arr, [swap_c(v) for v in out[:3]], out[3:])
        return (y_out, x_grad, *grads, g_sh_gate, g_sh_up, g_sh_down, g_router)

    return jax.shard_map(local_work, mesh=mesh, in_specs=in_specs, out_specs=out_specs, check_vma=False)
```

```python
import functools

import jax
import jax.numpy as jnp
from jax import lax
from jax.experimental import pallas as pl
from jax.experimental.pallas import tpu as pltpu
from jax.sharding import PartitionSpec as P


EPS = 1e-5
F32 = jnp.float32
BF16 = jnp.bfloat16
SPLIT = (2, 3, 3)
WIDTH_STEPS = 2
TOKEN_TILE = 512
GRAD_TILE = 1024
TOKEN_PARTS = 2
PICK_STEPS = 2


def glu_parts(d_hidden, act_gate, act_up):
    sig = 0.5 * jnp.tanh(0.5 * act_gate) + 0.5
    silu = act_gate * sig
    hidden = (silu * act_up).astype(BF16)
    d_gate = (d_hidden * act_up * (sig + silu * (1.0 - sig))).astype(BF16)
    return hidden, d_gate, (d_hidden * silu).astype(BF16)


def dot_nn(a, b):
    return lax.dot_general(a, b, (((1,), (0,)), ((), ())), preferred_element_type=F32)


def dot_nt(a, b):
    return lax.dot_general(a, b, (((1,), (1,)), ((), ())), preferred_element_type=F32)


def dot_tn(a, b):
    return lax.dot_general(a, b, (((0,), (0,)), ((), ())), preferred_element_type=F32)


def expert_kernel(kind, n_alias, rank_ref, x_ref, u_ref, wg_ref, wu_ref, wd_ref, *rest):
    rest = rest[n_alias:]
    if kind != "rows":
        gwg_ref, gwu_ref, gwd_ref = rest[:3]
        rest = rest[3:]
    rows, cot = x_ref[0], u_ref[0]
    wg, wu, wd = wg_ref[0], wu_ref[0], wd_ref[0]
    act_gate = dot_nn(rows, wg)
    act_up = dot_nn(rows, wu)
    d_hidden = dot_nt(cot, wd)
    hidden, d_gate, d_up = glu_parts(d_hidden, act_gate, act_up)
    if kind != "rows":
        gwd_ref[0] = dot_tn(hidden, cot)
        gwg_ref[0] = dot_tn(rows, d_gate)
        gwu_ref[0] = dot_tn(rows, d_up)
    if kind == "grads":
        return
    keep_ref, send_ref, o_acc, dn_acc = rest
    step = pl.program_id(1)
    last = pl.num_programs(1) - 1
    o_part = dot_nn(hidden, wd)
    dn_part = dot_nt(d_gate, wg) + dot_nt(d_up, wu)

    @pl.when(step == 0)
    def _():
        o_acc[...] = o_part
        dn_acc[...] = dn_part

    @pl.when(step > 0)
    def _():
        o_acc[...] += o_part
        dn_acc[...] += dn_part

    split_cols((step == last), rank_ref[0], o_acc, dn_acc, keep_ref, send_ref)


def split_cols(when, etp, out, dn, keep_ref, send_ref):
    half = out.shape[1] // 2

    @pl.when(when & (etp == 0))
    def _():
        keep_ref[:, :half] = out[:, :half]
        keep_ref[:, half:] = dn[:, :half]
        send_ref[:, :half] = out[:, half:]
        send_ref[:, half:] = dn[:, half:]

    @pl.when(when & (etp == 1))
    def _():
        keep_ref[:, :half] = out[:, half:]
        keep_ref[:, half:] = dn[:, half:]
        send_ref[:, :half] = out[:, :half]
        send_ref[:, half:] = dn[:, :half]


def expert_chunk(kind, first, count, rank, rows, cot, wg, wu, wd, grads):
    num, dim, width = wg.shape
    cap = rows.shape[1]
    tile = width // WIDTH_STEPS
    any_spec = pl.BlockSpec(memory_space=pl.ANY)
    row_spec = pl.BlockSpec((1, cap, dim), lambda e, f: (first + e, 0, 0))
    in_spec = pl.BlockSpec((1, dim, tile), lambda e, f: (first + e, 0, f))
    down_spec = pl.BlockSpec((1, tile, dim), lambda e, f: (first + e, f, 0))
    out_specs, out_shape, scratch = [], [], []
    if kind != "rows":
        out_specs += [in_spec, in_spec, down_spec]
        out_shape += [jax.ShapeDtypeStruct(v, F32) for v in ((num, dim, width), (num, dim, width), (num, width, dim))]
    if kind != "grads":
        out_specs += [pl.BlockSpec((cap, dim), lambda e, f: (e, 0))] * 2
        out_shape += [jax.ShapeDtypeStruct((count * cap, dim), F32)] * 2
        scratch = [pltpu.VMEM((cap, dim), F32)] * 2
    n_alias = len(grads)
    dots = 9 if kind == "all" else 6
    return pl.pallas_call(
        functools.partial(expert_kernel, kind, n_alias),
        grid=(count, WIDTH_STEPS),
        in_specs=[pl.BlockSpec(memory_space=pltpu.SMEM), row_spec, row_spec, in_spec, in_spec, down_spec] + [any_spec] * n_alias,
        out_specs=out_specs,
        out_shape=out_shape,
        scratch_shapes=scratch,
        input_output_aliases={6 + i: i for i in range(n_alias)},
        compiler_params=pltpu.CompilerParams(dimension_semantics=("arbitrary", "arbitrary"), vmem_limit_bytes=56 * 1024 * 1024),
        cost_estimate=pl.CostEstimate(flops=dots * 2 * count * cap * dim * width, bytes_accessed=count * 3 * dim * width * 6, transcendentals=0),
    )(rank, rows, cot, wg, wu, wd, *grads)


def shared_tokens_kernel(etp_ref, n_ref, dy_ref, wg_ref, wu_ref, wd_ref, keep_ref, send_ref):
    rows, cot = n_ref[...], dy_ref[...]
    tile = wg_ref.shape[1] // 2
    out = dn = None
    for i in range(2):
        cols = slice(i * tile, (i + 1) * tile)
        wg, wu, wd = wg_ref[:, cols], wu_ref[:, cols], wd_ref[cols, :]
        hidden, d_gate, d_up = glu_parts(dot_nt(cot, wd), dot_nn(rows, wg), dot_nn(rows, wu))
        out_part = dot_nn(hidden, wd)
        dn_part = dot_nt(d_gate, wg) + dot_nt(d_up, wu)
        out, dn = (out_part, dn_part) if i == 0 else (out + out_part, dn + dn_part)
    split_cols(pl.program_id(0) >= 0, etp_ref[0], out, dn, keep_ref, send_ref)


def shared_tokens(etp, n, dy, weights):
    tokens, dim = n.shape
    width = weights[0].shape[1]
    row = pl.BlockSpec((TOKEN_TILE, dim), lambda j: (j, 0))
    one = pl.Buffered(1)
    wide = pl.BlockSpec((dim, width), lambda j: (0, 0), pipeline_mode=one)
    tall = pl.BlockSpec((width, dim), lambda j: (0, 0), pipeline_mode=one)
    return pl.pallas_call(
        shared_tokens_kernel,
        grid=(tokens // TOKEN_TILE,),
        in_specs=[pl.BlockSpec(memory_space=pltpu.SMEM), row, row, wide, wide, tall],
        out_specs=[row, row],
        out_shape=[jax.ShapeDtypeStruct((tokens, dim), F32)] * 2,
        compiler_params=pltpu.CompilerParams(dimension_semantics=("arbitrary",), vmem_limit_bytes=60 * 1024 * 1024),
        cost_estimate=pl.CostEstimate(flops=12 * tokens * dim * width, bytes_accessed=16 * 1024 * 1024, transcendentals=0),
        name="shared_tokens",
    )(etp, n, dy, *weights)


def shared_kernel(mode, ids_ref, n_a, n_b, dy_a, dy_b, wg_ref, wu_ref, wd_ref, *rest):
    first_half = pl.program_id(0) == 0
    start = first_half & (pl.program_id(1) == 0)
    if mode == 0:
        gg_ref, gu_ref, gd_ref = rest
    else:
        pg_ref, pu_ref, pd_ref, gg_ref, gu_ref, gd_ref, fg_ref, fu_ref, fd_ref = rest
    rows = jnp.where(first_half, n_a[...], n_b[...])
    cot = jnp.where(first_half, dy_a[...], dy_b[...])
    wg, wu, wd = wg_ref[...], wu_ref[...], wd_ref[...]
    part = rows.shape[0] // TOKEN_PARTS
    acts = []
    for i in range(TOKEN_PARTS):
        own, own_cot = rows[i * part : (i + 1) * part], cot[i * part : (i + 1) * part]
        acts.append((dot_nt(own_cot, wd), dot_nn(own, wg), dot_nn(own, wu)))
    hidden, d_gate, d_up = [jnp.concatenate(v, axis=0) for v in zip(*[glu_parts(*v) for v in acts])]

    @pl.when(start)
    def _():
        gg_ref[...] = pg_ref[...] if mode else jnp.zeros_like(gg_ref)
        gu_ref[...] = pu_ref[...] if mode else jnp.zeros_like(gu_ref)
        gd_ref[...] = pd_ref[...] if mode else jnp.zeros_like(gd_ref)

    gg_ref[...] += dot_tn(rows, d_gate)
    gu_ref[...] += dot_tn(rows, d_up)
    gd_ref[...] += dot_tn(hidden, cot)
    if mode == 1:
        @pl.when(jnp.logical_not(first_half) & (pl.program_id(1) == pl.num_programs(1) - 1))
        def _():
            fg_ref[...] = gg_ref[...]
            fu_ref[...] = gu_ref[...]
            fd_ref[...] = gd_ref[...]


def shared_pass(mode, ids, n_pair, dy_pair, weights, earlier=()):
    tokens, dim = n_pair[0].shape
    tok = GRAD_TILE
    width = weights[0].shape[1]
    tile = width // 2
    steps = tokens // tok
    one = pl.Buffered(1)
    early = pl.BlockSpec((tok, dim), lambda h, j, ids: (jnp.where(h == 0, j, steps - 1), 0))
    late = pl.BlockSpec((tok, dim), lambda h, j, ids: (jnp.where(h == 0, 0, j), 0))
    col = pl.BlockSpec((dim, tile), lambda h, j, ids: (0, ids[0]), pipeline_mode=one)
    row = pl.BlockSpec((tile, dim), lambda h, j, ids: (ids[0], 0), pipeline_mode=one)
    sums = [(dim, tile), (dim, tile), (tile, dim)]
    sum_specs = [pl.BlockSpec(v, lambda h, j, ids: (0, 0), pipeline_mode=one) for v in sums]
    sum_shapes = [jax.ShapeDtypeStruct(v, F32) for v in sums]
    in_specs = [early, late, early, late, col, col, row]
    if mode == 0:
        out_specs, out_shape = sum_specs, sum_shapes
    else:
        in_specs += sum_specs
        out_specs = sum_specs + [col, col, row]
        out_shape = sum_shapes + [jax.ShapeDtypeStruct(v, F32) for v in ((dim, width), (dim, width), (width, dim))]
    return pl.pallas_call(
        functools.partial(shared_kernel, mode),
        grid_spec=pltpu.PrefetchScalarGridSpec(num_scalar_prefetch=1, grid=(2, steps), in_specs=in_specs, out_specs=out_specs),
        out_shape=out_shape,
        compiler_params=pltpu.CompilerParams(dimension_semantics=("arbitrary", "arbitrary"), vmem_limit_bytes=60 * 1024 * 1024),
        cost_estimate=pl.CostEstimate(flops=24 * tokens * dim * tile, bytes_accessed=30 * 1024 * 1024, transcendentals=0),
    )(ids, *n_pair, *dy_pair, *weights, *earlier)


def place_kernel(core_ref, a_ref, b_ref, c_ref, ah, bh, ch, ao_ref, bo_ref, co_ref):
    ao_ref[...] = a_ref[...]
    bo_ref[...] = b_ref[...]
    co_ref[...] = c_ref[...]


def place_halves(core, parts, whole):
    dim, tile = parts[0].shape
    steps = 4
    any_spec = pl.BlockSpec(memory_space=pl.ANY)
    in_row = pl.BlockSpec((dim // steps, tile), lambda j, core: (j, 0))
    down_row = pl.BlockSpec((tile // steps, dim), lambda j, core: (j, 0))
    out_col = pl.BlockSpec((dim // steps, tile), lambda j, core: (j, 1 - core[0]))
    out_row = pl.BlockSpec((tile // steps, dim), lambda j, core: ((1 - core[0]) * steps + j, 0))
    return pl.pallas_call(
        place_kernel,
        grid_spec=pltpu.PrefetchScalarGridSpec(num_scalar_prefetch=1, grid=(steps,), in_specs=[in_row, in_row, down_row] + [any_spec] * 3, out_specs=[out_col, out_col, out_row]),
        out_shape=[jax.ShapeDtypeStruct(w.shape, F32) for w in whole],
        input_output_aliases={4: 0, 5: 1, 6: 2},
        cost_estimate=pl.CostEstimate(flops=1000000, bytes_accessed=15 * 1024 * 1024, transcendentals=0),
        name="place",
    )(core, *parts, *whole)


def pick_kernel(with_gate, cap, tgt_ref, *refs):
    if with_gate:
        wr_ref, first_ref, *srcs, out, g_ref = refs
    else:
        g_ref, *srcs, out = refs
    tok = srcs[0].shape[0]
    slots = out.shape[0]
    slot = lax.broadcasted_iota(jnp.int32, (slots, tok), 0) + pl.program_id(0) * slots
    got = None
    for i, src in enumerate(srcs):
        term = dot_nn((tgt_ref[:, i * tok : (i + 1) * tok] == slot).astype(BF16), src[...])
        got = term if got is None else got + term
    if not with_gate:
        out[...] = (g_ref[...] * got).astype(BF16)
        return
    rows = got.astype(BF16)
    out[...] = rows
    logits = dot_nn(rows, wr_ref[...])
    grow = jnp.exp(logits - jnp.max(logits, axis=1, keepdims=True))
    probs = grow / jnp.sum(grow, axis=1, keepdims=True)
    lane = lax.broadcasted_iota(jnp.int32, logits.shape, 1)
    index = lax.broadcasted_iota(jnp.int32, logits.shape, 0)
    expert = first_ref[0] + pl.program_id(0) * (slots // cap)
    for k in range(1, slots // cap):
        expert = expert + (index >= k * cap).astype(jnp.int32)
    g_ref[...] = jnp.sum(jnp.where(lane == expert, probs, 0.0), axis=1, keepdims=True)


def pick_rows(target, blocks, slots, cap, gate=None, router=None):
    tok, dim = blocks[0].shape
    tile = slots // PICK_STEPS
    whole = pl.BlockSpec((tok, dim), lambda e: (0, 0), pipeline_mode=pl.Buffered(1))
    row_spec = pl.BlockSpec((tile, dim), lambda e: (e, 0))
    g_spec = pl.BlockSpec((tile, 1), lambda e: (e, 0))
    row_shape, g_shape = jax.ShapeDtypeStruct((slots, dim), BF16), jax.ShapeDtypeStruct((slots, 1), F32)
    if router is None:
        extra, extra_specs, out_specs, out_shape = [gate], [g_spec], row_spec, row_shape
    else:
        extra = list(router)
        extra_specs = [pl.BlockSpec(router[0].shape, lambda e: (0, 0)), pl.BlockSpec(memory_space=pltpu.SMEM)]
        out_specs, out_shape = [row_spec, g_spec], [row_shape, g_shape]
    return pl.pallas_call(
        functools.partial(pick_kernel, router is not None, cap),
        grid=(PICK_STEPS,),
        in_specs=[pl.BlockSpec((1, len(blocks) * tok), lambda e: (0, 0))] + extra_specs + [whole] * len(blocks),
        out_specs=out_specs,
        out_shape=out_shape,
        compiler_params=pltpu.CompilerParams(dimension_semantics=("arbitrary",), vmem_limit_bytes=48 * 1024 * 1024),
        cost_estimate=pl.CostEstimate(flops=2 * slots * len(blocks) * tok * dim, bytes_accessed=8 * 1024 * 1024, transcendentals=0),
        name="pick",
    )(target, *extra, *blocks)


def join_kernel(etp_ref, *refs):
    n = len(refs) // 3
    for i in range(n):
        mine, other, out = refs[2 * i], refs[2 * i + 1], refs[2 * n + i]
        half = mine.shape[1]

        @pl.when(etp_ref[0] == 0)
        def _():
            out[:, :half] = mine[...]
            out[:, half:] = other[...]

        @pl.when(etp_ref[0] == 1)
        def _():
            out[:, :half] = other[...]
            out[:, half:] = mine[...]


def join_cols(etp, pairs):
    tokens, half = pairs[0][0].shape
    tok = tokens // 2
    spec = pl.BlockSpec((tok, half), lambda j: (j, 0))
    return pl.pallas_call(
        join_kernel,
        grid=(2,),
        in_specs=[pl.BlockSpec(memory_space=pltpu.SMEM)] + [spec] * (2 * len(pairs)),
        out_specs=[pl.BlockSpec((tok, 2 * half), lambda j: (j, 0))] * len(pairs),
        out_shape=[jax.ShapeDtypeStruct((tokens, 2 * half), BF16)] * len(pairs),
        cost_estimate=pl.CostEstimate(flops=1000000, bytes_accessed=6 * 1024 * 1024, transcendentals=0),
        name="join",
    )(etp, *[v for p in pairs for v in p])


def exclusive_rank(onehot):
    num, tokens = onehot.shape
    blk = 256
    nb = tokens // blk
    below = (jnp.arange(blk)[:, None] < jnp.arange(blk)[None, :]).astype(BF16)
    parts = onehot.reshape(num * nb, blk)
    local = dot_nn(parts, below).reshape(num, nb, blk)
    sums = jnp.sum(parts.astype(F32), axis=1).reshape(num, nb)
    earlier = (jnp.arange(nb)[:, None] < jnp.arange(nb)[None, :]).astype(F32)
    base = jnp.sum(sums[:, :, None] * earlier[None], axis=1)
    ranks = (local + base[:, :, None]).reshape(num, tokens)
    rank = jnp.sum(ranks * onehot.astype(F32), axis=0)
    return rank, jnp.sum(sums, axis=1)


def solution(mesh):
    ep_size = mesh.shape["ep"]
    tok_spec = P(("dp", "ep"), None)
    id_spec = P(("dp", "ep"))
    in_specs = (tok_spec, tok_spec, id_spec, id_spec, P(None, None), P("ep", None, "etp"), P("ep", None, "etp"), P("ep", "etp", None), P(None, "etp"), P(None, "etp"), P("etp", None))
    out_specs = (tok_spec, tok_spec, P(("dp", "ep"), None, "etp"), P(("dp", "ep"), None, "etp"), P(("dp", "ep"), "etp", None), P("dp", "etp"), P("dp", "etp"), P(("dp", "etp"), None), P("dp", None))
    swap_x = lambda v: lax.ppermute(v, "ep", [(i, i ^ 2) for i in range(ep_size)])
    swap_c = lambda v: lax.ppermute(v, "ep", [(i, i ^ 1) for i in range(ep_size)])
    swap_y = lambda v: lax.ppermute(v, "etp", [(0, 1), (1, 0)])

    def spread(v):
        far = swap_x(v)
        return [v, swap_c(v), far, swap_c(far)]

    def local_work(x_in, y_grad, prim_exp, alt_exp, w_router, exp_gate, exp_up, exp_down, sh_gate, sh_up, sh_down):
        tok_local, model_dim = x_in.shape
        num_exp = w_router.shape[1]
        local_exp = exp_gate.shape[0]
        capacity = 5 * tok_local * ep_size // (4 * num_exp)
        local_slots = local_exp * capacity
        half = model_dim // 2
        rank = lax.axis_index("ep")
        etp = lax.axis_index("etp")
        my_col = etp * half
        cols = lambda v: lax.dynamic_slice_in_dim(v, my_col, half, 1)

        x_wide = x_in.astype(F32)
        inv_rms = lax.rsqrt(jnp.mean(x_wide * x_wide, axis=1, keepdims=True) + EPS)
        normed = (x_wide * inv_rms).astype(BF16)
        ids = spread(jnp.stack([prim_exp, alt_exp]))
        dy_blocks = spread(y_grad)
        n_blocks = spread(normed)

        core = rank % 2
        ids_arr = jnp.stack([core, etp]).astype(jnp.int32)
        etp_arr = ids_arr[1:]
        sh_weights = (sh_gate, sh_up, sh_down)
        sh_keep, sh_send = shared_tokens(etp_arr, normed, y_grad, sh_weights)
        sh_recv = swap_y(sh_send)
        sh_sums = shared_pass(0, ids_arr, n_blocks[:2], dy_blocks[:2], sh_weights)
        sh_half = sh_keep + sh_recv
        sh_out, dn_shared = sh_half[:, :half], sh_half[:, half:]

        ids_all = jnp.take(jnp.stack(ids), rank ^ jnp.arange(ep_size), axis=0)
        prim_all = ids_all[:, 0, :].reshape(1, -1)
        alt_all = ids_all[:, 1, :].reshape(1, -1)
        expert_col = jnp.arange(num_exp)[:, None]
        one_prim = (prim_all == expert_col).astype(BF16)
        rank_prim, prim_counts = exclusive_rank(one_prim)
        keep_prim = rank_prim < capacity
        kept = jnp.minimum(prim_counts, float(capacity))
        one_alt = ((alt_all == expert_col) & jnp.logical_not(keep_prim)[None, :]).astype(BF16)
        rank_alt, _ = exclusive_rank(one_alt)
        slot_alt = rank_alt + jnp.sum(one_alt.astype(F32) * kept[:, None], axis=0)
        keep_alt = jnp.logical_not(keep_prim) & (slot_alt < capacity)
        assign = jnp.where(keep_prim, prim_all[0], jnp.where(keep_alt, alt_all[0], num_exp))
        slot = jnp.where(keep_prim, rank_prim, jnp.where(keep_alt, slot_alt, 0.0)).astype(jnp.int32)
        pos = (assign * capacity + slot).reshape(ep_size, tok_local)
        pos_blocks = jnp.take(pos, rank ^ jnp.arange(ep_size), axis=0)
        pos_own = pos_blocks[0]
        assign_own = lax.dynamic_slice_in_dim(assign.reshape(ep_size, tok_local), rank, 1, 0).reshape(tok_local, 1)

        gate_probs = jax.nn.softmax(dot_nn(normed, w_router), axis=1)
        one_assign = (assign_own == jnp.arange(num_exp)[None, :]).astype(F32)
        gate_val = jnp.sum(gate_probs * one_assign, axis=1, keepdims=True)

        target = pos_blocks.reshape(1, -1) - rank * local_slots
        rows, g_slot = pick_rows(target, n_blocks, local_slots, capacity, router=(w_router, (rank * local_exp).reshape(1).astype(jnp.int32)))
        cot = pick_rows(target, dy_blocks, local_slots, capacity, gate=g_slot)
        rows = rows.reshape(local_exp, capacity, model_dim)
        cot = cot.reshape(local_exp, capacity, model_dim)

        grads = ()
        picked = jnp.zeros((tok_local, model_dim), F32)
        pos_col = pos_own.reshape(tok_local, 1)
        first = 0
        for per in SPLIT:
            work = (first, per, etp_arr, rows, cot, exp_gate, exp_up, exp_down)
            *grads, keep, send = expert_chunk("all", *work, grads)
            final = (keep + swap_y(send)).astype(BF16)
            blocks = jnp.concatenate(spread(final), axis=0)
            owner = rank ^ jnp.arange(ep_size)
            ids_row = (owner[:, None] * local_slots + first * capacity + jnp.arange(per * capacity)[None, :]).reshape(1, -1)
            picked = picked + dot_nn((pos_col == ids_row).astype(BF16), blocks)
            first += per
        tok_out, dn_routed = picked[:, :half], picked[:, half:]

        x_half, dy_half = cols(x_in).astype(F32), cols(y_grad).astype(F32)
        y_half = (x_half + sh_out + gate_val * tok_out).astype(BF16)
        dg_part = jnp.sum(dy_half * tok_out, axis=1).reshape(1, tok_local)
        d_gate_val = (dg_part + swap_y(dg_part)).reshape(tok_local, 1)
        d_logits = (d_gate_val * gate_val * (one_assign - gate_probs)).astype(BF16)
        router_part = dot_tn(d_logits, normed)
        router_part = router_part + swap_c(router_part)
        g_router = (router_part + swap_x(router_part)).T
        dn_router = dot_nt(d_logits, lax.dynamic_slice_in_dim(w_router, my_col, half, 0))
        d_normed = dn_shared + dn_router + dn_routed
        proj_part = jnp.sum(d_normed * x_half, axis=1).reshape(1, tok_local)
        norm_proj = ((proj_part + swap_y(proj_part)) / model_dim).reshape(tok_local, 1)
        xg_half = (dy_half + inv_rms * d_normed - x_half * inv_rms ** 3 * norm_proj).astype(BF16)

        y_recv = swap_y(y_half)
        xg_recv = swap_y(xg_half)
        y_out, x_grad = join_cols(etp_arr, [(y_half, y_recv), (xg_half, xg_recv)])

        out = shared_pass(1, ids_arr, n_blocks[2:], dy_blocks[2:], sh_weights, sh_sums)
        others = [swap_c(v) for v in out[:3]]
        g_sh_gate, g_sh_up, g_sh_down = place_halves(ids_arr, others, out[3:])
        return (y_out, x_grad, *grads, g_sh_gate, g_sh_up, g_sh_down, g_router)

    return jax.shard_map(local_work, mesh=mesh, in_specs=in_specs, out_specs=out_specs, check_vma=False)
```

```python
import functools

import jax
import jax.numpy as jnp
from jax import lax
from jax.experimental import pallas as pl
from jax.experimental.pallas import tpu as pltpu
from jax.sharding import PartitionSpec as P


EPS = 1e-5
F32 = jnp.float32
BF16 = jnp.bfloat16
SPLIT = (2, 3, 3)
WIDTH_STEPS = 2
TOKEN_TILE = 512
GRAD_TILE = 512
TOKEN_PARTS = 2
PICK_STEPS = 2


def glu_parts(d_hidden, act_gate, act_up):
    sig = 0.5 * jnp.tanh(0.5 * act_gate) + 0.5
    silu = act_gate * sig
    hidden = (silu * act_up).astype(BF16)
    d_gate = (d_hidden * act_up * (sig + silu * (1.0 - sig))).astype(BF16)
    return hidden, d_gate, (d_hidden * silu).astype(BF16)


def dot_nn(a, b):
    return lax.dot_general(a, b, (((1,), (0,)), ((), ())), preferred_element_type=F32)


def dot_nt(a, b):
    return lax.dot_general(a, b, (((1,), (1,)), ((), ())), preferred_element_type=F32)


def dot_tn(a, b):
    return lax.dot_general(a, b, (((0,), (0,)), ((), ())), preferred_element_type=F32)


def expert_kernel(kind, n_alias, rank_ref, x_ref, u_ref, wg_ref, wu_ref, wd_ref, *rest):
    rest = rest[n_alias:]
    if kind != "rows":
        gwg_ref, gwu_ref, gwd_ref = rest[:3]
        rest = rest[3:]
    rows, cot = x_ref[0], u_ref[0]
    wg, wu, wd = wg_ref[0], wu_ref[0], wd_ref[0]
    act_gate = dot_nn(rows, wg)
    act_up = dot_nn(rows, wu)
    d_hidden = dot_nt(cot, wd)
    hidden, d_gate, d_up = glu_parts(d_hidden, act_gate, act_up)
    if kind != "rows":
        gwd_ref[0] = dot_tn(hidden, cot)
        gwg_ref[0] = dot_tn(rows, d_gate)
        gwu_ref[0] = dot_tn(rows, d_up)
    if kind == "grads":
        return
    keep_ref, send_ref, o_acc, dn_acc = rest
    step = pl.program_id(1)
    last = pl.num_programs(1) - 1
    o_part = dot_nn(hidden, wd)
    dn_part = dot_nt(d_gate, wg) + dot_nt(d_up, wu)

    @pl.when(step == 0)
    def _():
        o_acc[...] = o_part
        dn_acc[...] = dn_part

    @pl.when(step > 0)
    def _():
        o_acc[...] += o_part
        dn_acc[...] += dn_part

    split_cols((step == last), rank_ref[0], o_acc, dn_acc, keep_ref, send_ref)


def split_cols(when, etp, out, dn, keep_ref, send_ref):
    half = out.shape[1] // 2

    @pl.when(when & (etp == 0))
    def _():
        keep_ref[:, :half] = out[:, :half]
        keep_ref[:, half:] = dn[:, :half]
        send_ref[:, :half] = out[:, half:]
        send_ref[:, half:] = dn[:, half:]

    @pl.when(when & (etp == 1))
    def _():
        keep_ref[:, :half] = out[:, half:]
        keep_ref[:, half:] = dn[:, half:]
        send_ref[:, :half] = out[:, :half]
        send_ref[:, half:] = dn[:, :half]


def expert_chunk(kind, first, count, rank, rows, cot, wg, wu, wd, grads):
    num, dim, width = wg.shape
    cap = rows.shape[1]
    tile = width // WIDTH_STEPS
    any_spec = pl.BlockSpec(memory_space=pl.ANY)
    row_spec = pl.BlockSpec((1, cap, dim), lambda e, f: (first + e, 0, 0))
    in_spec = pl.BlockSpec((1, dim, tile), lambda e, f: (first + e, 0, f))
    down_spec = pl.BlockSpec((1, tile, dim), lambda e, f: (first + e, f, 0))
    out_specs, out_shape, scratch = [], [], []
    if kind != "rows":
        out_specs += [in_spec, in_spec, down_spec]
        out_shape += [jax.ShapeDtypeStruct(v, F32) for v in ((num, dim, width), (num, dim, width), (num, width, dim))]
    if kind != "grads":
        out_specs += [pl.BlockSpec((cap, dim), lambda e, f: (e, 0))] * 2
        out_shape += [jax.ShapeDtypeStruct((count * cap, dim), F32)] * 2
        scratch = [pltpu.VMEM((cap, dim), F32)] * 2
    n_alias = len(grads)
    dots = 9 if kind == "all" else 6
    return pl.pallas_call(
        functools.partial(expert_kernel, kind, n_alias),
        grid=(count, WIDTH_STEPS),
        in_specs=[pl.BlockSpec(memory_space=pltpu.SMEM), row_spec, row_spec, in_spec, in_spec, down_spec] + [any_spec] * n_alias,
        out_specs=out_specs,
        out_shape=out_shape,
        scratch_shapes=scratch,
        input_output_aliases={6 + i: i for i in range(n_alias)},
        compiler_params=pltpu.CompilerParams(dimension_semantics=("arbitrary", "arbitrary"), vmem_limit_bytes=56 * 1024 * 1024),
        cost_estimate=pl.CostEstimate(flops=dots * 2 * count * cap * dim * width, bytes_accessed=count * 3 * dim * width * 6, transcendentals=0),
    )(rank, rows, cot, wg, wu, wd, *grads)


def shared_tokens_kernel(etp_ref, n_ref, dy_ref, wg_ref, wu_ref, wd_ref, keep_ref, send_ref):
    rows, cot = n_ref[...], dy_ref[...]
    tile = wg_ref.shape[1] // 2
    out = dn = None
    for i in range(2):
        cols = slice(i * tile, (i + 1) * tile)
        wg, wu, wd = wg_ref[:, cols], wu_ref[:, cols], wd_ref[cols, :]
        hidden, d_gate, d_up = glu_parts(dot_nt(cot, wd), dot_nn(rows, wg), dot_nn(rows, wu))
        out_part = dot_nn(hidden, wd)
        dn_part = dot_nt(d_gate, wg) + dot_nt(d_up, wu)
        out, dn = (out_part, dn_part) if i == 0 else (out + out_part, dn + dn_part)
    split_cols(pl.program_id(0) >= 0, etp_ref[0], out, dn, keep_ref, send_ref)


def shared_tokens(etp, n, dy, weights):
    tokens, dim = n.shape
    width = weights[0].shape[1]
    row = pl.BlockSpec((TOKEN_TILE, dim), lambda j: (j, 0))
    one = pl.Buffered(1)
    wide = pl.BlockSpec((dim, width), lambda j: (0, 0), pipeline_mode=one)
    tall = pl.BlockSpec((width, dim), lambda j: (0, 0), pipeline_mode=one)
    return pl.pallas_call(
        shared_tokens_kernel,
        grid=(tokens // TOKEN_TILE,),
        in_specs=[pl.BlockSpec(memory_space=pltpu.SMEM), row, row, wide, wide, tall],
        out_specs=[row, row],
        out_shape=[jax.ShapeDtypeStruct((tokens, dim), F32)] * 2,
        compiler_params=pltpu.CompilerParams(dimension_semantics=("arbitrary",), vmem_limit_bytes=60 * 1024 * 1024),
        cost_estimate=pl.CostEstimate(flops=12 * tokens * dim * width, bytes_accessed=16 * 1024 * 1024, transcendentals=0),
        name="shared_tokens",
    )(etp, n, dy, *weights)


def shared_kernel(mode, ids_ref, n_a, n_b, dy_a, dy_b, wg_ref, wu_ref, wd_ref, *rest):
    first_half = pl.program_id(0) == 0
    start = first_half & (pl.program_id(1) == 0)
    if mode == 0:
        gg_ref, gu_ref, gd_ref = rest
    else:
        pg_ref, pu_ref, pd_ref, gg_ref, gu_ref, gd_ref, fg_ref, fu_ref, fd_ref = rest
    rows = jnp.where(first_half, n_a[...], n_b[...])
    cot = jnp.where(first_half, dy_a[...], dy_b[...])
    wg, wu, wd = wg_ref[...], wu_ref[...], wd_ref[...]
    part = rows.shape[0] // TOKEN_PARTS
    acts = []
    for i in range(TOKEN_PARTS):
        own, own_cot = rows[i * part : (i + 1) * part], cot[i * part : (i + 1) * part]
        acts.append((dot_nt(own_cot, wd), dot_nn(own, wg), dot_nn(own, wu)))
    hidden, d_gate, d_up = [jnp.concatenate(v, axis=0) for v in zip(*[glu_parts(*v) for v in acts])]

    @pl.when(start)
    def _():
        gg_ref[...] = pg_ref[...] if mode else jnp.zeros_like(gg_ref)
        gu_ref[...] = pu_ref[...] if mode else jnp.zeros_like(gu_ref)
        gd_ref[...] = pd_ref[...] if mode else jnp.zeros_like(gd_ref)

    gg_ref[...] += dot_tn(rows, d_gate)
    gu_ref[...] += dot_tn(rows, d_up)
    gd_ref[...] += dot_tn(hidden, cot)
    if mode == 1:
        @pl.when(jnp.logical_not(first_half) & (pl.program_id(1) == pl.num_programs(1) - 1))
        def _():
            fg_ref[...] = gg_ref[...]
            fu_ref[...] = gu_ref[...]
            fd_ref[...] = gd_ref[...]


def shared_pass(mode, ids, n_pair, dy_pair, weights, earlier=()):
    tokens, dim = n_pair[0].shape
    tok = GRAD_TILE
    width = weights[0].shape[1]
    tile = width // 2
    steps = tokens // tok
    one = pl.Buffered(1)
    early = pl.BlockSpec((tok, dim), lambda h, j, ids: (jnp.where(h == 0, j, steps - 1), 0))
    late = pl.BlockSpec((tok, dim), lambda h, j, ids: (jnp.where(h == 0, 0, j), 0))
    col = pl.BlockSpec((dim, tile), lambda h, j, ids: (0, ids[0]), pipeline_mode=one)
    row = pl.BlockSpec((tile, dim), lambda h, j, ids: (ids[0], 0), pipeline_mode=one)
    sums = [(dim, tile), (dim, tile), (tile, dim)]
    sum_specs = [pl.BlockSpec(v, lambda h, j, ids: (0, 0), pipeline_mode=one) for v in sums]
    sum_shapes = [jax.ShapeDtypeStruct(v, F32) for v in sums]
    in_specs = [early, late, early, late, col, col, row]
    if mode == 0:
        out_specs, out_shape = sum_specs, sum_shapes
    else:
        in_specs += sum_specs
        out_specs = sum_specs + [col, col, row]
        out_shape = sum_shapes + [jax.ShapeDtypeStruct(v, F32) for v in ((dim, width), (dim, width), (width, dim))]
    return pl.pallas_call(
        functools.partial(shared_kernel, mode),
        grid_spec=pltpu.PrefetchScalarGridSpec(num_scalar_prefetch=1, grid=(2, steps), in_specs=in_specs, out_specs=out_specs),
        out_shape=out_shape,
        compiler_params=pltpu.CompilerParams(dimension_semantics=("arbitrary", "arbitrary"), vmem_limit_bytes=60 * 1024 * 1024),
        cost_estimate=pl.CostEstimate(flops=24 * tokens * dim * tile, bytes_accessed=30 * 1024 * 1024, transcendentals=0),
    )(ids, *n_pair, *dy_pair, *weights, *earlier)


def place_kernel(core_ref, a_ref, b_ref, c_ref, ah, bh, ch, ao_ref, bo_ref, co_ref):
    ao_ref[...] = a_ref[...]
    bo_ref[...] = b_ref[...]
    co_ref[...] = c_ref[...]


def place_halves(core, parts, whole):
    dim, tile = parts[0].shape
    steps = 4
    any_spec = pl.BlockSpec(memory_space=pl.ANY)
    in_row = pl.BlockSpec((dim // steps, tile), lambda j, core: (j, 0))
    down_row = pl.BlockSpec((tile // steps, dim), lambda j, core: (j, 0))
    out_col = pl.BlockSpec((dim // steps, tile), lambda j, core: (j, 1 - core[0]))
    out_row = pl.BlockSpec((tile // steps, dim), lambda j, core: ((1 - core[0]) * steps + j, 0))
    return pl.pallas_call(
        place_kernel,
        grid_spec=pltpu.PrefetchScalarGridSpec(num_scalar_prefetch=1, grid=(steps,), in_specs=[in_row, in_row, down_row] + [any_spec] * 3, out_specs=[out_col, out_col, out_row]),
        out_shape=[jax.ShapeDtypeStruct(w.shape, F32) for w in whole],
        input_output_aliases={4: 0, 5: 1, 6: 2},
        cost_estimate=pl.CostEstimate(flops=1000000, bytes_accessed=15 * 1024 * 1024, transcendentals=0),
        name="place",
    )(core, *parts, *whole)


def pick_kernel(kind, cap, tgt_ref, *refs):
    if kind == "gate":
        wr_ref, first_ref, *srcs, out, g_ref = refs
    elif kind == "scale":
        g_ref, start_ref, *srcs, out = refs
    else:
        *srcs, out = refs
    tok = srcs[0].shape[0]
    slots = out.shape[0]
    base = pl.program_id(0) * slots
    slot = lax.broadcasted_iota(jnp.int32, (slots, tok), 0) + base
    got = start_ref[...].astype(F32) if kind == "scale" else None
    for i, src in enumerate(srcs):
        term = dot_nn((tgt_ref[:, i * tok : (i + 1) * tok] == slot).astype(BF16), src[...])
        got = term if got is None else got + term
    if kind == "scale":
        got = g_ref[...] * got
    rows = got.astype(BF16)
    out[...] = rows
    if kind != "gate":
        return
    logits = dot_nn(rows, wr_ref[...])
    grow = jnp.exp(logits - jnp.max(logits, axis=1, keepdims=True))
    probs = grow / jnp.sum(grow, axis=1, keepdims=True)
    lane = lax.broadcasted_iota(jnp.int32, logits.shape, 1)
    index = lax.broadcasted_iota(jnp.int32, logits.shape, 0) + base
    expert = first_ref[0]
    for k in range(1, PICK_STEPS * slots // cap):
        expert = expert + (index >= k * cap).astype(jnp.int32)
    g_ref[...] = jnp.sum(jnp.where(lane == expert, probs, 0.0), axis=1, keepdims=True)


def pick_rows(kind, target, blocks, slots, cap, extra=()):
    tok, dim = blocks[0].shape
    tile = slots // PICK_STEPS
    whole = pl.BlockSpec((tok, dim), lambda e: (0, 0), pipeline_mode=pl.Buffered(1))
    row_spec = pl.BlockSpec((tile, dim), lambda e: (e, 0))
    g_spec = pl.BlockSpec((tile, 1), lambda e: (e, 0))
    row_shape, g_shape = jax.ShapeDtypeStruct((slots, dim), BF16), jax.ShapeDtypeStruct((slots, 1), F32)
    out_specs, out_shape, extra_specs = [row_spec], [row_shape], []
    if kind == "scale":
        extra_specs = [g_spec, row_spec]
    if kind == "gate":
        extra_specs = [pl.BlockSpec(extra[0].shape, lambda e: (0, 0)), pl.BlockSpec(memory_space=pltpu.SMEM)]
        out_specs, out_shape = [row_spec, g_spec], [row_shape, g_shape]
    return pl.pallas_call(
        functools.partial(pick_kernel, kind, cap),
        grid=(PICK_STEPS,),
        in_specs=[pl.BlockSpec((1, len(blocks) * tok), lambda e: (0, 0))] + extra_specs + [whole] * len(blocks),
        out_specs=out_specs,
        out_shape=out_shape,
        compiler_params=pltpu.CompilerParams(dimension_semantics=("arbitrary",), vmem_limit_bytes=48 * 1024 * 1024),
        cost_estimate=pl.CostEstimate(flops=2 * slots * len(blocks) * tok * dim, bytes_accessed=8 * 1024 * 1024, transcendentals=0),
    )(target, *extra, *blocks)


def join_kernel(etp_ref, *refs):
    n = len(refs) // 3
    for i in range(n):
        mine, other, out = refs[2 * i], refs[2 * i + 1], refs[2 * n + i]
        half = mine.shape[1]

        @pl.when(etp_ref[0] == 0)
        def _():
            out[:, :half] = mine[...]
            out[:, half:] = other[...]

        @pl.when(etp_ref[0] == 1)
        def _():
            out[:, :half] = other[...]
            out[:, half:] = mine[...]


def join_cols(etp, pairs):
    tokens, half = pairs[0][0].shape
    tok = tokens // 2
    spec = pl.BlockSpec((tok, half), lambda j: (j, 0))
    return pl.pallas_call(
        join_kernel,
        grid=(2,),
        in_specs=[pl.BlockSpec(memory_space=pltpu.SMEM)] + [spec] * (2 * len(pairs)),
        out_specs=[pl.BlockSpec((tok, 2 * half), lambda j: (j, 0))] * len(pairs),
        out_shape=[jax.ShapeDtypeStruct((tokens, 2 * half), BF16)] * len(pairs),
        cost_estimate=pl.CostEstimate(flops=1000000, bytes_accessed=6 * 1024 * 1024, transcendentals=0),
        name="join",
    )(etp, *[v for p in pairs for v in p])


def exclusive_rank(onehot):
    num, tokens = onehot.shape
    blk = 256
    nb = tokens // blk
    below = (jnp.arange(blk)[:, None] < jnp.arange(blk)[None, :]).astype(BF16)
    parts = onehot.reshape(num * nb, blk)
    local = dot_nn(parts, below).reshape(num, nb, blk)
    sums = jnp.sum(parts.astype(F32), axis=1).reshape(num, nb)
    earlier = (jnp.arange(nb)[:, None] < jnp.arange(nb)[None, :]).astype(F32)
    base = jnp.sum(sums[:, :, None] * earlier[None], axis=1)
    ranks = (local + base[:, :, None]).reshape(num, tokens)
    rank = jnp.sum(ranks * onehot.astype(F32), axis=0)
    return rank, jnp.sum(sums, axis=1)


def solution(mesh):
    ep_size = mesh.shape["ep"]
    tok_spec = P(("dp", "ep"), None)
    id_spec = P(("dp", "ep"))
    in_specs = (tok_spec, tok_spec, id_spec, id_spec, P(None, None), P("ep", None, "etp"), P("ep", None, "etp"), P("ep", "etp", None), P(None, "etp"), P(None, "etp"), P("etp", None))
    out_specs = (tok_spec, tok_spec, P(("dp", "ep"), None, "etp"), P(("dp", "ep"), None, "etp"), P(("dp", "ep"), "etp", None), P("dp", "etp"), P("dp", "etp"), P(("dp", "etp"), None), P("dp", None))
    swap_x = lambda v: lax.ppermute(v, "ep", [(i, i ^ 2) for i in range(ep_size)])
    swap_c = lambda v: lax.ppermute(v, "ep", [(i, i ^ 1) for i in range(ep_size)])
    swap_y = lambda v: lax.ppermute(v, "etp", [(0, 1), (1, 0)])

    def spread(v):
        far = swap_x(v)
        return [v, swap_c(v), far, swap_c(far)]

    def local_work(x_in, y_grad, prim_exp, alt_exp, w_router, exp_gate, exp_up, exp_down, sh_gate, sh_up, sh_down):
        tok_local, model_dim = x_in.shape
        num_exp = w_router.shape[1]
        local_exp = exp_gate.shape[0]
        capacity = 5 * tok_local * ep_size // (4 * num_exp)
        local_slots = local_exp * capacity
        half = model_dim // 2
        rank = lax.axis_index("ep")
        etp = lax.axis_index("etp")
        my_col = etp * half
        cols = lambda v: lax.dynamic_slice_in_dim(v, my_col, half, 1)

        x_wide = x_in.astype(F32)
        inv_rms = lax.rsqrt(jnp.mean(x_wide * x_wide, axis=1, keepdims=True) + EPS)
        normed = (x_wide * inv_rms).astype(BF16)
        ids = spread(jnp.stack([prim_exp, alt_exp]))
        dy_blocks = spread(y_grad)
        n_blocks = spread(normed)

        core = rank % 2
        ids_arr = jnp.stack([core, etp]).astype(jnp.int32)
        etp_arr = ids_arr[1:]
        sh_weights = (sh_gate, sh_up, sh_down)
        sh_keep, sh_send = shared_tokens(etp_arr, normed, y_grad, sh_weights)
        sh_recv = swap_y(sh_send)
        sh_sums = shared_pass(0, ids_arr, n_blocks[:2], dy_blocks[:2], sh_weights)
        sh_half = sh_keep + sh_recv
        sh_out, dn_shared = sh_half[:, :half], sh_half[:, half:]

        ids_all = jnp.take(jnp.stack(ids), rank ^ jnp.arange(ep_size), axis=0)
        prim_all = ids_all[:, 0, :].reshape(1, -1)
        alt_all = ids_all[:, 1, :].reshape(1, -1)
        expert_col = jnp.arange(num_exp)[:, None]
        one_prim = (prim_all == expert_col).astype(BF16)
        rank_prim, prim_counts = exclusive_rank(one_prim)
        keep_prim = rank_prim < capacity
        kept = jnp.minimum(prim_counts, float(capacity))
        one_alt = ((alt_all == expert_col) & jnp.logical_not(keep_prim)[None, :]).astype(BF16)
        rank_alt, _ = exclusive_rank(one_alt)
        slot_alt = rank_alt + jnp.sum(one_alt.astype(F32) * kept[:, None], axis=0)
        keep_alt = jnp.logical_not(keep_prim) & (slot_alt < capacity)
        assign = jnp.where(keep_prim, prim_all[0], jnp.where(keep_alt, alt_all[0], num_exp))
        slot = jnp.where(keep_prim, rank_prim, jnp.where(keep_alt, slot_alt, 0.0)).astype(jnp.int32)
        pos = (assign * capacity + slot).reshape(ep_size, tok_local)
        pos_blocks = jnp.take(pos, rank ^ jnp.arange(ep_size), axis=0)
        pos_own = pos_blocks[0]
        assign_own = lax.dynamic_slice_in_dim(assign.reshape(ep_size, tok_local), rank, 1, 0).reshape(tok_local, 1)

        gate_probs = jax.nn.softmax(dot_nn(normed, w_router), axis=1)
        one_assign = (assign_own == jnp.arange(num_exp)[None, :]).astype(F32)
        gate_val = jnp.sum(gate_probs * one_assign, axis=1, keepdims=True)

        target = pos_blocks.reshape(1, -1) - rank * local_slots
        near, far = target[:, : 2 * tok_local], target[:, 2 * tok_local :]
        rows, g_slot = pick_rows("gate", target, n_blocks, local_slots, capacity, (w_router, (rank * local_exp).reshape(1).astype(jnp.int32)))
        (cot,) = pick_rows("plain", near, dy_blocks[:2], local_slots, capacity)
        (cot,) = pick_rows("scale", far, dy_blocks[2:], local_slots, capacity, (g_slot, cot))
        rows = rows.reshape(local_exp, capacity, model_dim)
        cot = cot.reshape(local_exp, capacity, model_dim)

        grads = ()
        picked = jnp.zeros((tok_local, model_dim), F32)
        pos_col = pos_own.reshape(tok_local, 1)
        first = 0
        for c, per in enumerate(SPLIT):
            work = (first, per, etp_arr, rows, cot, exp_gate, exp_up, exp_down)
            *grads, keep, send = expert_chunk("all", *work, grads)
            final = (keep + swap_y(send)).astype(BF16)
            owner = rank ^ jnp.arange(ep_size)
            ids_row = (owner[:, None] * local_slots + first * capacity + jnp.arange(per * capacity)[None, :]).reshape(1, -1)
            hits = (pos_col == ids_row).astype(BF16)
            first += per
            if c < len(SPLIT) - 1:
                blocks = jnp.concatenate(spread(final), axis=0)
                picked = picked + dot_nn(hits, blocks)
        out_blocks = jnp.concatenate(spread(final[:, :half]), axis=0)
        dn_blocks = jnp.concatenate(spread(final[:, half:]), axis=0)
        tok_out = picked[:, :half] + dot_nn(hits, out_blocks)
        dn_routed = picked[:, half:] + dot_nn(hits, dn_blocks)

        x_half, dy_half = cols(x_in).astype(F32), cols(y_grad).astype(F32)
        y_half = (x_half + sh_out + gate_val * tok_out).astype(BF16)
        dg_part = jnp.sum(dy_half * tok_out, axis=1).reshape(1, tok_local)
        y_half, dg_part = lax.optimization_barrier((y_half, dg_part))
        d_gate_val = (dg_part + swap_y(dg_part)).reshape(tok_local, 1)
        d_logits = (d_gate_val * gate_val * (one_assign - gate_probs)).astype(BF16)
        router_part = dot_tn(d_logits, normed)
        router_part = router_part + swap_c(router_part)
        g_router = (router_part + swap_x(router_part)).T
        dn_router = dot_nt(d_logits, lax.dynamic_slice_in_dim(w_router, my_col, half, 0))
        d_normed = dn_shared + dn_router + dn_routed
        proj_part = jnp.sum(d_normed * x_half, axis=1).reshape(1, tok_local)
        norm_proj = ((proj_part + swap_y(proj_part)) / model_dim).reshape(tok_local, 1)
        xg_half = (dy_half + inv_rms * d_normed - x_half * inv_rms ** 3 * norm_proj).astype(BF16)

        cut = tok_local // 2
        y_recv = jnp.concatenate([swap_y(y_half[:cut]), swap_y(y_half[cut:])], axis=0)
        xg_recv = swap_y(xg_half)
        (y_out,) = join_cols(etp_arr, [(y_half, y_recv)])
        (x_grad,) = join_cols(etp_arr, [(xg_half, xg_recv)])

        out = shared_pass(1, ids_arr, n_blocks[2:], dy_blocks[2:], sh_weights, sh_sums)
        others = [swap_c(v) for v in out[:3]]
        g_sh_gate, g_sh_up, g_sh_down = place_halves(ids_arr, others, out[3:])
        return (y_out, x_grad, *grads, g_sh_gate, g_sh_up, g_sh_down, g_router)

    return jax.shard_map(local_work, mesh=mesh, in_specs=in_specs, out_specs=out_specs, check_vma=False)
```
